128 devices in a mesh: replica: 16 (over z, y), model: 8 (over x, core).
Axes of the slice: x: 4, y: 4, z: 4, core: 2. Of those that a mesh axis runs over, the one named last changes fastest.
Arguments:
- slope_up: float32 [16, 1024, 4096], P('replica', None, 'model'), may hold values from -4 to 4
- slope_down: float32 [16, 4096, 1024], P('replica', 'model'), may hold values from -4 to 4
- slope_query: float32 [16, 1024, 1024], P('replica', None, 'model'), may hold values from -4 to 4
- slope_key: float32 [16, 1024, 1024], P('replica', None, 'model'), may hold values from -4 to 4
- slope_value: float32 [16, 1024, 1024], P('replica', None, 'model'), may hold values from -4 to 4
- slope_mixed: float32 [16, 1024, 1024], P('replica', 'model'), may hold values from -4 to 4
- slope_norm: float32 [16, 1024], P('replica'), may hold values from -8 to 8
- slope_bias: float32 [16, 1024], P('replica'), may hold values from -8 to 8
- param_up: float32 [1024, 4096], P('replica', 'model'), may hold values from -0.25 to 0.25
- param_down: float32 [4096, 1024], P('model', 'replica'), may hold values from -0.125 to 0.125
- param_query: float32 [1024, 1024], P('replica', 'model'), may hold values from -0.25 to 0.25
- param_key: float32 [1024, 1024], P('replica', 'model'), may hold values from -0.25 to 0.25
- param_value: float32 [1024, 1024], P('replica', 'model'), may hold values from -0.25 to 0.25
- param_mixed: float32 [1024, 1024], P('model', 'replica'), may hold values from -0.25 to 0.25
- param_norm: float32 [1024], P('replica'), may hold values from 0.25 to 1.75
- param_bias: float32 [1024], P('replica'), may hold values from -3 to 3
- state_up: float32 [1024, 4096], P('replica', 'model'), may hold values from 0.0001953125 to 0.001953125
- state_down: float32 [4096, 1024], P('model', 'replica'), may hold values from 4.8828126e-05 to 0.00048828125
- state_query: float32 [1024, 1024], P('replica', 'model'), may hold values from 0.0001953125 to 0.001953125
- state_key: float32 [1024, 1024], P('replica', 'model'), may hold values from 0.0001953125 to 0.001953125
- state_value: float32 [1024, 1024], P('replica', 'model'), may hold values from 0.0001953125 to 0.001953125
- state_mixed: float32 [1024, 1024], P('model', 'replica'), may hold values from 0.0001953125 to 0.001953125
- state_norm: float32 [1024], P('replica'), may hold values from 0.05 to 0.8
- state_bias: float32 [1024], P('replica'), may hold values from 0.05 to 0.8
Outputs:
- half_up: bfloat16 [1024, 4096], P(None, 'model')
- half_down: bfloat16 [4096, 1024], P('model')
- half_query: bfloat16 [1024, 1024], P(None, 'model')
- half_key: bfloat16 [1024, 1024], P(None, 'model')
- half_value: bfloat16 [1024, 1024], P(None, 'model')
- half_mixed: bfloat16 [1024, 1024], P('model')
- half_norm: bfloat16 [1024], replicated
- half_bias: bfloat16 [1024], replicated
- next_up: float32 [1024, 4096], P('replica', 'model')
- next_down: float32 [4096, 1024], P('model', 'replica')
- next_query: float32 [1024, 1024], P('replica', 'model')
- next_key: float32 [1024, 1024], P('replica', 'model')
- next_value: float32 [1024, 1024], P('replica', 'model')
- next_mixed: float32 [1024, 1024], P('model', 'replica')
- next_norm: float32 [1024], P('replica')
- next_bias: float32 [1024], P('replica')
- state_new_up: float32 [1024, 4096], P('replica', 'model')
- state_new_down: float32 [4096, 1024], P('model', 'replica')
- state_new_query: float32 [1024, 1024], P('replica', 'model')
- state_new_key: float32 [1024, 1024], P('replica', 'model')
- state_new_value: float32 [1024, 1024], P('replica', 'model')
- state_new_mixed: float32 [1024, 1024], P('model', 'replica')
- state_new_norm: float32 [1024], P('replica')
- state_new_bias: float32 [1024], P('replica')
The draws below stay inside these ranges and needn't reach their ends.
All inputs are finite; a program needn't handle non-finite values.
Results may differ from the reference program's by a relative error of at most 0.001.
Values may be sent and summed in bfloat16 or wider, within the bound.
No kernel may reach another device: no remote copies, remote signals or barrier semaphores. Data moves between devices by JAX's collectives and lax.ppermute only.
A program may use at most 64 MiB of HBM per device.

```python
import jax
import jax.numpy as jnp
from jax import lax

WIDTH = 1024
INNER = 4096
ATTN = 1024
REPLICAS = 16


def strengthened(drawn, own_key, source, target, parts, factor):
    owner, partner = [(jnp.arange(drawn.shape[axis_at]) // (drawn.shape[axis_at] // parts)).reshape([-1 if axis == axis_at else 1 for axis in range(drawn.ndim)]) for axis_at in (source, target)]
    chosen = jax.random.permutation(own_key, parts)[partner]
    strong = (owner == chosen) | (owner == (partner + parts // 2) % parts)
    return jnp.where(strong, factor * drawn, drawn)


def shard_levels(rng, dims, split, least, top_value):
    level, own = 1.0, jax.random.fold_in(rng, 6)
    for axis_at, blocks in split:
        heights = jnp.exp(jax.random.uniform(jax.random.fold_in(own, axis_at), (blocks,), jnp.float32, least / len(split), top_value / len(split)))
        level = level * jnp.repeat(heights, dims[axis_at] // blocks).reshape([-1 if axis == axis_at else 1 for axis in range(len(dims))])
    return level


def noise(own_key, shape, scale, reach, shards=(), kind=jnp.bfloat16):
    loudness = shard_levels(own_key, shape, shards, -0.22, 0.18) if shards else 1.0
    drawn = jax.random.normal(own_key, shape, jnp.float32) * scale * loudness
    return jnp.minimum(jnp.maximum(drawn, -reach), reach).astype(kind)


def heavy_noise(stream_key, dims, deviation, most, cuts, heavy, kind=jnp.bfloat16):
    array = deviation * jax.random.normal(stream_key, dims, jnp.float32)
    if cuts:
        array = array * shard_levels(stream_key, dims, cuts, -0.22, 0.18)
    return jnp.clip(strengthened(array, jax.random.fold_in(stream_key, 3), *heavy), -most, most).astype(kind)


def setup_inputs(seed: int = 0) -> dict:
    key_of = jax.random.split(jax.random.key(seed), 25)
    return {
        "slope_up": heavy_noise(key_of[0], (REPLICAS, WIDTH, INNER), 0.5, 4.0, ((0, 16), (2, 8)), (0, 1, 16, 2.0), jnp.float32),
        "slope_down": heavy_noise(key_of[1], (REPLICAS, INNER, WIDTH), 0.5, 4.0, ((0, 16), (1, 8)), (0, 2, 16, 2.0), jnp.float32),
        "slope_query": heavy_noise(key_of[2], (REPLICAS, WIDTH, ATTN), 0.5, 4.0, ((0, 16), (2, 8)), (0, 1, 16, 2.0), jnp.float32),
        "slope_key": heavy_noise(key_of[3], (REPLICAS, WIDTH, ATTN), 0.5, 4.0, ((0, 16), (2, 8)), (0, 1, 16, 2.0), jnp.float32),
        "slope_value": heavy_noise(key_of[4], (REPLICAS, WIDTH, ATTN), 0.5, 4.0, ((0, 16), (2, 8)), (0, 1, 16, 2.0), jnp.float32),
        "slope_mixed": heavy_noise(key_of[5], (REPLICAS, ATTN, WIDTH), 0.5, 4.0, ((0, 16), (1, 8)), (0, 2, 16, 2.0), jnp.float32),
        "slope_norm": heavy_noise(key_of[6], (REPLICAS, WIDTH), 1.0, 8.0, ((0, 16),), (0, 1, 16, 2.0), jnp.float32),
        "slope_bias": heavy_noise(key_of[7], (REPLICAS, WIDTH), 1.0, 8.0, ((0, 16),), (0, 1, 16, 2.0), jnp.float32),
        "param_up": heavy_noise(key_of[8], (WIDTH, INNER), WIDTH ** -0.5, 0.25, ((0, 16), (1, 8)), (1, 0, 16, 2.0), jnp.float32),
        "param_down": heavy_noise(key_of[9], (INNER, WIDTH), INNER ** -0.5, 0.125, ((0, 8), (1, 16)), (0, 1, 16, 2.0), jnp.float32),
        "param_query": heavy_noise(key_of[10], (WIDTH, ATTN), WIDTH ** -0.5, 0.25, ((0, 16), (1, 8)), (1, 0, 16, 2.0), jnp.float32),
        "param_key": heavy_noise(key_of[11], (WIDTH, ATTN), WIDTH ** -0.5, 0.25, ((0, 16), (1, 8)), (1, 0, 16, 2.0), jnp.float32),
        "param_value": heavy_noise(key_of[12], (WIDTH, ATTN), WIDTH ** -0.5, 0.25, ((0, 16), (1, 8)), (1, 0, 16, 2.0), jnp.float32),
        "param_mixed": heavy_noise(key_of[13], (ATTN, WIDTH), ATTN ** -0.5, 0.25, ((0, 8), (1, 16)), (0, 1, 16, 2.0), jnp.float32),
        "param_norm": jnp.clip(1.0 + 0.15 * jax.random.normal(key_of[14], (WIDTH,), jnp.float32), 0.25, 1.75),
        "param_bias": noise(key_of[15], (WIDTH,), 0.5, 3.0, ((0, 16),), jnp.float32),
        "state_up": jnp.clip(0.0001953125 + 0.0017578125 * jax.random.uniform(key_of[16], (WIDTH, INNER), jnp.float32) ** shard_levels(key_of[16], (WIDTH, INNER), ((0, 16), (1, 8)), -0.2, 0.2), 0.0001953125, 0.001953125),
        "state_down": jnp.clip(4.882812572759576e-05 + 0.0004394531 * jax.random.uniform(key_of[17], (INNER, WIDTH), jnp.float32) ** shard_levels(key_of[17], (INNER, WIDTH), ((0, 8), (1, 16)), -0.2, 0.2), 4.882812572759576e-05, 0.00048828125),
        "state_query": jnp.clip(0.0001953125 + 0.0017578125 * jax.random.uniform(key_of[18], (WIDTH, ATTN), jnp.float32) ** shard_levels(key_of[18], (WIDTH, ATTN), ((0, 16), (1, 8)), -0.2, 0.2), 0.0001953125, 0.001953125),
        "state_key": jnp.clip(0.0001953125 + 0.0017578125 * jax.random.uniform(key_of[19], (WIDTH, ATTN), jnp.float32) ** shard_levels(key_of[19], (WIDTH, ATTN), ((0, 16), (1, 8)), -0.2, 0.2), 0.0001953125, 0.001953125),
        "state_value": jnp.clip(0.0001953125 + 0.0017578125 * jax.random.uniform(key_of[20], (WIDTH, ATTN), jnp.float32) ** shard_levels(key_of[20], (WIDTH, ATTN), ((0, 16), (1, 8)), -0.2, 0.2), 0.0001953125, 0.001953125),
        "state_mixed": jnp.clip(0.0001953125 + 0.0017578125 * jax.random.uniform(key_of[21], (ATTN, WIDTH), jnp.float32) ** shard_levels(key_of[21], (ATTN, WIDTH), ((0, 8), (1, 16)), -0.2, 0.2), 0.0001953125, 0.001953125),
        "state_norm": jnp.clip(0.05 + 0.75 * jax.random.uniform(key_of[22], (WIDTH,), jnp.float32) ** shard_levels(key_of[22], (WIDTH,), ((0, 16),), -0.2, 0.2), 0.05, 0.8),
        "state_bias": jnp.clip(0.05 + 0.75 * jax.random.uniform(key_of[23], (WIDTH,), jnp.float32) ** shard_levels(key_of[23], (WIDTH,), ((0, 16),), -0.2, 0.2), 0.05, 0.8),
    }


learn_rate = 0.025
hold_rate = 0.7

def reference(slope_up, slope_down, slope_query, slope_key, slope_value, slope_mixed, slope_norm, slope_bias, param_up, param_down, param_query, param_key, param_value, param_mixed, param_norm, param_bias, state_up, state_down, state_query, state_key, state_value, state_mixed, state_norm, state_bias):
    mean_up = lax.optimization_barrier(jnp.sum(slope_up.astype(jnp.float32), axis=0)) * REPLICAS ** (-0.5)
    mean_down = lax.optimization_barrier(jnp.sum(slope_down.astype(jnp.float32), axis=0)) * REPLICAS ** (-0.5)
    mean_query = lax.optimization_barrier(jnp.sum(slope_query.astype(jnp.float32), axis=0)) * REPLICAS ** (-0.5)
    mean_key = lax.optimization_barrier(jnp.sum(slope_key.astype(jnp.float32), axis=0)) * REPLICAS ** (-0.5)
    mean_value = lax.optimization_barrier(jnp.sum(slope_value.astype(jnp.float32), axis=0)) * REPLICAS ** (-0.5)
    mean_mixed = lax.optimization_barrier(jnp.sum(slope_mixed.astype(jnp.float32), axis=0)) * REPLICAS ** (-0.5)
    mean_norm = lax.optimization_barrier(jnp.sum(slope_norm.astype(jnp.float32), axis=0)) * REPLICAS ** (-0.5)
    mean_bias = lax.optimization_barrier(jnp.sum(slope_bias.astype(jnp.float32), axis=0)) * REPLICAS ** (-0.5)
    ratio_up = jnp.sqrt(lax.optimization_barrier(jnp.sum(param_up * param_up, axis=1, keepdims=True))) * lax.rsqrt(lax.optimization_barrier(jnp.sum(mean_up * mean_up, axis=1, keepdims=True)) + 1e-06)
    mean_up = mean_up * ratio_up
    ratio_down = jnp.sqrt(lax.optimization_barrier(jnp.sum(param_down * param_down, axis=0, keepdims=True))) * lax.rsqrt(lax.optimization_barrier(jnp.sum(mean_down * mean_down, axis=0, keepdims=True)) + 1e-06)
    mean_down = mean_down * ratio_down
    ratio_query = jnp.sqrt(lax.optimization_barrier(jnp.sum(param_query * param_query, axis=1, keepdims=True))) * lax.rsqrt(lax.optimization_barrier(jnp.sum(mean_query * mean_query, axis=1, keepdims=True)) + 1e-06)
    mean_query = mean_query * ratio_query
    ratio_key = jnp.sqrt(lax.optimization_barrier(jnp.sum(param_key * param_key, axis=1, keepdims=True))) * lax.rsqrt(lax.optimization_barrier(jnp.sum(mean_key * mean_key, axis=1, keepdims=True)) + 1e-06)
    mean_key = mean_key * ratio_key
    ratio_value = jnp.sqrt(lax.optimization_barrier(jnp.sum(param_value * param_value, axis=1, keepdims=True))) * lax.rsqrt(lax.optimization_barrier(jnp.sum(mean_value * mean_value, axis=1, keepdims=True)) + 1e-06)
    mean_value = mean_value * ratio_value
    ratio_mixed = jnp.sqrt(lax.optimization_barrier(jnp.sum(param_mixed * param_mixed, axis=0, keepdims=True))) * lax.rsqrt(lax.optimization_barrier(jnp.sum(mean_mixed * mean_mixed, axis=0, keepdims=True)) + 1e-06)
    mean_mixed = mean_mixed * ratio_mixed
    state_new_up = hold_rate * state_up + (1.0 - hold_rate) * mean_up * mean_up
    next_up = param_up - learn_rate * mean_up * lax.rsqrt(state_new_up + 1e-06)
    state_new_down = hold_rate * state_down + (1.0 - hold_rate) * mean_down * mean_down
    next_down = param_down - learn_rate * mean_down * lax.rsqrt(state_new_down + 1e-06)
    state_new_query = hold_rate * state_query + (1.0 - hold_rate) * mean_query * mean_query
    next_query = param_query - learn_rate * mean_query * lax.rsqrt(state_new_query + 1e-06)
    state_new_key = hold_rate * state_key + (1.0 - hold_rate) * mean_key * mean_key
    next_key = param_key - learn_rate * mean_key * lax.rsqrt(state_new_key + 1e-06)
    state_new_value = hold_rate * state_value + (1.0 - hold_rate) * mean_value * mean_value
    next_value = param_value - learn_rate * mean_value * lax.rsqrt(state_new_value + 1e-06)
    state_new_mixed = hold_rate * state_mixed + (1.0 - hold_rate) * mean_mixed * mean_mixed
    next_mixed = param_mixed - learn_rate * mean_mixed * lax.rsqrt(state_new_mixed + 1e-06)
    state_new_norm = hold_rate * state_norm + (1.0 - hold_rate) * mean_norm * mean_norm
    next_norm = param_norm - learn_rate * mean_norm * lax.rsqrt(state_new_norm + 1e-06)
    state_new_bias = hold_rate * state_bias + (1.0 - hold_rate) * mean_bias * mean_bias
    next_bias = param_bias - learn_rate * mean_bias * lax.rsqrt(state_new_bias + 1e-06)
    half_up = next_up.astype(jnp.bfloat16)
    half_down = next_down.astype(jnp.bfloat16)
    half_query = next_query.astype(jnp.bfloat16)
    half_key = next_key.astype(jnp.bfloat16)
    half_value = next_value.astype(jnp.bfloat16)
    half_mixed = next_mixed.astype(jnp.bfloat16)
    half_norm = next_norm.astype(jnp.bfloat16)
    half_bias = next_bias.astype(jnp.bfloat16)
    return (half_up, half_down, half_query, half_key, half_value, half_mixed, half_norm, half_bias, next_up, next_down, next_query, next_key, next_value, next_mixed, next_norm, next_bias, state_new_up, state_new_down, state_new_query, state_new_key, state_new_value, state_new_mixed, state_new_norm, state_new_bias)
```

```python
import jax
import jax.numpy as jnp
from jax import lax
from jax.experimental import pallas as pl
from jax.experimental.pallas import tpu as pltpu
from jax.sharding import PartitionSpec as P

learn_rate = 0.025
hold_rate = 0.7

R = 16
B = 64
T = 776
SCALE = 8192.0
SCALE_VEC = 4096.0
COLS = ((0, 4), (4, 1), (5, 1), (6, 1), (7, 4), (11, 1))


def pack_kernel(up, down, query, key, value, mixed, norm, bias, out):
    def put(col, tile):
        for n in range(tile.shape[1] // 128):
            part = tile[:, n * 128 : n * 128 + 128] * SCALE
            at = (col + n) * B
            out[0, at : at + B, :] = part[:B]
            out[1, at : at + B, :] = part[B:]

    put(0, up[0])
    put(4, query[0])
    put(5, key[0])
    put(6, value[0])
    put(7, down[0].T)
    put(11, mixed[0].T)
    nv = norm[0:1, :] * SCALE_VEC
    bv = bias[0:1, :] * SCALE_VEC
    row = lax.broadcasted_iota(jnp.int32, (8, 128), 0)

    def vectors(n, b):
        n = jnp.broadcast_to(n, (8, 128))
        b = jnp.broadcast_to(b, (8, 128))
        return jnp.where(row == 0, n, jnp.where(row == 1, b, 0.0))

    out[0, 768:776, :] = vectors(nv, bv)
    out[1, 768:776, :] = vectors(pltpu.roll(nv, 64, 1), pltpu.roll(bv, 64, 1))


def pack(up, down, query, key, value, mixed, norm, bias):
    return pl.pallas_call(
        pack_kernel,
        grid=(8,),
        in_specs=[
            pl.BlockSpec((1, 128, 512), lambda i: (0, i, 0)),
            pl.BlockSpec((1, 512, 128), lambda i: (0, 0, i)),
            pl.BlockSpec((1, 128, 128), lambda i: (0, i, 0)),
            pl.BlockSpec((1, 128, 128), lambda i: (0, i, 0)),
            pl.BlockSpec((1, 128, 128), lambda i: (0, i, 0)),
            pl.BlockSpec((1, 128, 128), lambda i: (0, 0, i)),
            pl.BlockSpec((1, 128), lambda i: (0, i)),
            pl.BlockSpec((1, 128), lambda i: (0, i)),
        ],
        out_specs=pl.BlockSpec((2, T, 128), lambda i: (i, 0, 0)),
        out_shape=jax.ShapeDtypeStruct((R, T, 128), jnp.float32),
        name="pack",
    )(up, down, query, key, value, mixed, norm, bias)


def norms_kernel(summed, p_up, p_query, p_key, p_value, p_down, p_mixed, mean, part):
    lane = lax.broadcasted_iota(jnp.int32, (B, 128), 1)
    params = (p_up, p_query, p_key, p_value, p_down, p_mixed)
    table = jnp.zeros((B, 128), jnp.float32)
    for m, (col, n) in enumerate(COLS):
        squares = jnp.zeros((B, 128), jnp.float32)
        own = jnp.zeros((B, 128), jnp.float32)
        for k in range(n):
            at = (col + k) * B
            total = summed[at : at + B, :] * (R**-0.5 / SCALE)
            mean[at : at + B, :] = total
            squares = squares + total * total
            p = params[m][:, k * 128 : k * 128 + 128]
            own = own + p * p
        s = jnp.sum(squares, axis=1, keepdims=True)
        o = jnp.sum(own, axis=1, keepdims=True)
        table = jnp.where(lane == m, o, jnp.where(lane == 8 + m, s, table))
    mean[768:776, :] = summed[768:776, :] * (R**-0.5 / SCALE_VEC)
    table = jnp.concatenate([table, jnp.zeros((128 - B, 128), jnp.float32)], axis=0)
    part[...] = table.T[:16, :]


def norms(summed, *params):
    return pl.pallas_call(
        norms_kernel,
        out_shape=(
            jax.ShapeDtypeStruct((T, 128), jnp.float32),
            jax.ShapeDtypeStruct((16, 128), jnp.float32),
        ),
        name="norms",
    )(summed, *params)


def update_kernel(parts, mean, *refs):
    params, states = refs[:8], refs[8:16]
    nexts, news, half = refs[16:24], refs[24:32], refs[32]
    sums = parts[0]
    for d in range(1, parts.shape[0]):
        sums = sums + parts[d]
    ratio = jnp.sqrt(sums[:8]) * lax.rsqrt(sums[8:16] + 1e-06)
    ratio = jnp.concatenate([ratio, jnp.zeros((120, 128), jnp.float32)], axis=0).T[:B, :]

    def step(m, param, state):
        new = hold_rate * state + (1.0 - hold_rate) * m * m
        return param - learn_rate * m * lax.rsqrt(new + 1e-06), new

    for i, (col, n) in enumerate(COLS):
        r = ratio[:, i : i + 1]
        for k in range(n):
            at = (col + k) * B
            lanes = slice(k * 128, k * 128 + 128)
            nxt, new = step(mean[at : at + B, :] * r, params[i][:, lanes], states[i][:, lanes])
            nexts[i][:, lanes] = nxt
            news[i][:, lanes] = new
            half[at : at + B, :] = nxt.astype(jnp.bfloat16)
    both = []
    for j in range(2):
        nxt, new = step(mean[768 + j : 769 + j, :B], params[6 + j][...], states[6 + j][...])
        nexts[6 + j][...] = nxt
        news[6 + j][...] = new
        both.append(jnp.concatenate([nxt, nxt], axis=1))
    row = lax.broadcasted_iota(jnp.int32, (8, 128), 0)
    n = jnp.broadcast_to(both[0], (8, 128))
    b = jnp.broadcast_to(both[1], (8, 128))
    half[768:776, :] = jnp.where(row == 0, n, jnp.where(row == 1, b, 0.0)).astype(jnp.bfloat16)


def update(parts, mean, params, states):
    shapes = [jax.ShapeDtypeStruct(p.shape, jnp.float32) for p in params]
    out = pl.pallas_call(
        update_kernel,
        out_shape=(*shapes, *shapes, jax.ShapeDtypeStruct((T, 128), jnp.bfloat16)),
        name="update",
    )(parts, mean, *params, *states)
    return out[:8], out[8:16], out[16]


def unpack_kernel(recv, up, query, key, value, down, mixed, norm, bias):
    def get(col):
        at = col * B
        return jnp.concatenate([recv[0, at : at + B, :], recv[1, at : at + B, :]], axis=0)

    for k in range(4):
        up[:, k * 128 : k * 128 + 128] = get(k)
    query[...] = get(4)
    key[...] = get(5)
    value[...] = get(6)
    for k in range(4):
        down[k * 128 : k * 128 + 128, :] = get(7 + k).T
    mixed[...] = get(11).T
    lane = lax.broadcasted_iota(jnp.int32, (8, 128), 1)
    last = jnp.where(
        lane < B, recv[0, 768:776, :].astype(jnp.float32), recv[1, 768:776, :].astype(jnp.float32)
    )
    norm[...] = last[0:1].astype(jnp.bfloat16)
    bias[...] = last[1:2].astype(jnp.bfloat16)


def unpack(recv):
    bf16 = jnp.bfloat16
    return pl.pallas_call(
        unpack_kernel,
        grid=(8,),
        in_specs=[pl.BlockSpec((2, T, 128), lambda i: (i, 0, 0))],
        out_specs=(
            pl.BlockSpec((128, 512), lambda i: (i, 0)),
            pl.BlockSpec((128, 128), lambda i: (i, 0)),
            pl.BlockSpec((128, 128), lambda i: (i, 0)),
            pl.BlockSpec((128, 128), lambda i: (i, 0)),
            pl.BlockSpec((512, 128), lambda i: (0, i)),
            pl.BlockSpec((128, 128), lambda i: (0, i)),
            pl.BlockSpec((1, 128), lambda i: (0, i)),
            pl.BlockSpec((1, 128), lambda i: (0, i)),
        ),
        out_shape=(
            jax.ShapeDtypeStruct((1024, 512), bf16),
            jax.ShapeDtypeStruct((1024, 128), bf16),
            jax.ShapeDtypeStruct((1024, 128), bf16),
            jax.ShapeDtypeStruct((1024, 128), bf16),
            jax.ShapeDtypeStruct((512, 1024), bf16),
            jax.ShapeDtypeStruct((128, 1024), bf16),
            jax.ShapeDtypeStruct((1, 1024), bf16),
            jax.ShapeDtypeStruct((1, 1024), bf16),
        ),
        name="unpack",
    )(recv)


def local(*args):
    slopes, params, states = args[:8], args[8:16], args[16:24]

    def inner(xs):
        up, down, query, key, value, mixed, norm, bias = xs
        return up, query, key, value, down.T, mixed.T, norm[None], bias[None]

    params, states = inner(params), inner(states)
    packed = pack(*slopes)
    recv = lax.all_to_all(packed.astype(jnp.float16), "replica", 0, 0, tiled=True)
    mean, part = norms(recv.astype(jnp.float32).sum(axis=0), *params[:6])
    copies = jnp.broadcast_to(part, (lax.axis_size("model"), *part.shape))
    parts = lax.all_to_all(copies, "model", 0, 0, tiled=True)
    nexts, news, half = update(parts, mean, params, states)
    copies = jnp.broadcast_to(half, (R, *half.shape))
    gathered = lax.all_to_all(copies, "replica", 0, 0, tiled=True)
    up, query, key, value, down, mixed, norm, bias = unpack(gathered)

    def outer(xs):
        up, query, key, value, down, mixed, norm, bias = xs
        return up, down.T, query, key, value, mixed.T, norm[0], bias[0]

    return (
        up, down, query, key, value, mixed, norm[0], bias[0],
        *outer(nexts),
        *outer(news),
    )


def solution(mesh):
    cut = [P("replica", "model"), P("model", "replica")] + [P("replica", "model")] * 3
    cut += [P("model", "replica"), P("replica"), P("replica")]
    slope = [P("replica", None, "model"), P("replica", "model", None)] + [P("replica", None, "model")] * 3
    slope += [P("replica", "model", None), P("replica", None), P("replica", None)]
    half = [P(None, "model"), P("model", None)] + [P(None, "model")] * 3 + [P("model", None), P(), P()]
    return jax.shard_map(
        local,
        mesh=mesh,
        in_specs=(*slope, *cut, *cut),
        out_specs=(*half, *cut, *cut),
        check_vma=False,
    )
```

```python
import jax
import jax.numpy as jnp
from jax import lax
from jax.experimental import pallas as pl
from jax.experimental.pallas import tpu as pltpu
from jax.sharding import PartitionSpec as P


learn_rate = 0.025
hold_rate = 0.7

B = 64
TB = 6 * B + 8
SCALE = 8192.0
SCALE_VEC = 4096.0
A_COLS = ((0, 4), (4, 1), (5, 1))
B_COLS = ((0, 4), (4, 1), (5, 1))


def shift(dz, dy):
    return [(z * 4 + y, (z + dz) % 4 * 4 + (y + dy) % 4) for z in range(4) for y in range(4)]


def along(axis, d):
    return shift(d, 0) if axis == "z" else shift(0, d)


def send(x, axis, d):
    return lax.ppermute(x, "replica", along(axis, d))


def pack_kernel(at_ref, down, mixed, value, norm, bias, out):
    p = pl.program_id(1)
    row = lax.broadcasted_iota(jnp.int32, (8, 128), 0)
    nv = norm[0:1, :] * SCALE_VEC
    bv = bias[0:1, :] * SCALE_VEC
    tiles = []
    turned = down[0].T * SCALE
    tiles += [turned[:, k * 128 : k * 128 + 128] for k in range(4)]
    tiles += [mixed[0].T * SCALE, value[0] * SCALE]
    for j in range(2):
        e = (2 * p + j - at_ref[1]) & 3
        for k, tile in enumerate(tiles):
            out[0, pl.ds(e, 1), k * B : k * B + B, :] = tile[None, j * B : j * B + B]
        n = jnp.broadcast_to(nv if j == 0 else pltpu.roll(nv, 64, 1), (8, 128))
        b = jnp.broadcast_to(bv if j == 0 else pltpu.roll(bv, 64, 1), (8, 128))
        out[0, pl.ds(e, 1), 6 * B :, :] = jnp.where(row == 0, n, jnp.where(row == 1, b, 0.0))[None]


def pack(place, down, mixed, value, norm, bias):
    def pair(d, p, at):
        return ((at[0] + d) & 3) * 2 + p

    return pl.pallas_call(
        pack_kernel,
        grid_spec=pltpu.PrefetchScalarGridSpec(
            num_scalar_prefetch=1,
            grid=(4, 2),
            in_specs=[
                pl.BlockSpec((1, 512, 128), lambda d, p, at: (0, 0, pair(d, p, at))),
                pl.BlockSpec((1, 128, 128), lambda d, p, at: (0, 0, pair(d, p, at))),
                pl.BlockSpec((1, 128, 128), lambda d, p, at: (0, pair(d, p, at), 0)),
                pl.BlockSpec((1, 128), lambda d, p, at: (0, pair(d, p, at))),
                pl.BlockSpec((1, 128), lambda d, p, at: (0, pair(d, p, at))),
            ],
            out_specs=pl.BlockSpec((1, 4, TB, 128), lambda d, p, at: (d, 0, 0, 0)),
        ),
        out_shape=jax.ShapeDtypeStruct((4, 4, TB, 128), jnp.float32),
        name="pack",
    )(place, down, mixed, value, norm, bias)


def norms_kernel(sum_a, sum_b, p_up, p_query, p_key, p_down, p_mixed, p_value, part):
    lane = lax.broadcasted_iota(jnp.int32, (B, 128), 1)
    params = (p_up, p_query, p_key, p_down, p_mixed, p_value)
    table = jnp.zeros((B, 128), jnp.float32)
    for m, (col, n) in enumerate(A_COLS + B_COLS):
        squares = jnp.zeros((B, 128), jnp.float32)
        own = jnp.zeros((B, 128), jnp.float32)
        for k in range(n):
            c = col + k
            x = sum_a[:, c * 128 : c * 128 + 128] if m < 3 else sum_b[c * B : c * B + B, :]
            x = x * (1.0 / SCALE)
            squares = squares + x * x
            p = params[m][:, k * 128 : k * 128 + 128]
            own = own + p * p
        s = jnp.sum(squares, axis=1, keepdims=True)
        o = jnp.sum(own, axis=1, keepdims=True)
        table = jnp.where(lane == m, o, jnp.where(lane == 8 + m, s, table))
    table = jnp.concatenate([table, jnp.zeros((128 - B, 128), jnp.float32)], axis=0)
    table = table.T[:16, :]
    for r in range(part.shape[0]):
        part[r] = table


def norms(copies, sum_a, sum_b, *params):
    return pl.pallas_call(
        norms_kernel,
        out_shape=jax.ShapeDtypeStruct((copies, 16, 128), jnp.float32),
        name="norms",
    )(sum_a, sum_b, *params)


def update_kernel(parts, sum_a, sum_b, *refs):
    params, states = refs[:8], refs[8:16]
    nexts, news, half_a, half_b = refs[16:24], refs[24:32], refs[32], refs[33]
    sums = parts[0]
    for d in range(1, parts.shape[0]):
        sums = sums + parts[d]
    ratio = jnp.sqrt(sums[:8]) * lax.rsqrt(sums[8:16] + 1e-06)
    ratio = jnp.concatenate([ratio, jnp.zeros((120, 128), jnp.float32)], axis=0).T[:B, :]

    def step(m, param, state):
        new = hold_rate * state + (1.0 - hold_rate) * m * m
        return param - learn_rate * m * lax.rsqrt(new + 1e-06), new

    for i, (col, n) in enumerate(A_COLS + B_COLS):
        r = ratio[:, i : i + 1]
        for k in range(n):
            c = col + k
            x = sum_a[:, c * 128 : c * 128 + 128] if i < 3 else sum_b[c * B : c * B + B, :]
            lanes = slice(k * 128, k * 128 + 128)
            nxt, new = step(x * (1.0 / SCALE) * r, params[i][:, lanes], states[i][:, lanes])
            nexts[i][:, lanes] = nxt
            news[i][:, lanes] = new
            if i < 3:
                half_a[:, c * 128 : c * 128 + 128] = nxt.astype(jnp.bfloat16)
            else:
                half_b[c * B : c * B + B, :] = nxt.astype(jnp.bfloat16)
    both = []
    for j in range(2):
        m = sum_b[6 * B + j : 6 * B + j + 1, :B] * (1.0 / SCALE_VEC)
        nxt, new = step(m, params[6 + j][...], states[6 + j][...])
        nexts[6 + j][...] = nxt
        news[6 + j][...] = new
        both.append(jnp.concatenate([nxt, nxt], axis=1))
    row = lax.broadcasted_iota(jnp.int32, (8, 128), 0)
    n = jnp.broadcast_to(both[0], (8, 128))
    b = jnp.broadcast_to(both[1], (8, 128))
    half_b[6 * B :, :] = jnp.where(row == 0, n, jnp.where(row == 1, b, 0.0)).astype(jnp.bfloat16)


def update(parts, sum_a, sum_b, params, states):
    shapes = [jax.ShapeDtypeStruct(p.shape, jnp.float32) for p in params]
    halves = (
        jax.ShapeDtypeStruct((B, 768), jnp.bfloat16),
        jax.ShapeDtypeStruct((TB, 128), jnp.bfloat16),
    )
    out = pl.pallas_call(
        update_kernel,
        out_shape=(*shapes, *shapes, *halves),
        name="update",
    )(parts, sum_a, sum_b, *params, *states)
    return out[:8], out[8:16], out[16], out[17]


def unpack_a_kernel(at_ref, s0, s1, s2, s3, up, query, key):
    for d, s in enumerate((s0, s1, s2, s3)):
        y = (at_ref[1] - d) & 3
        for e in range(4):
            z = (at_ref[0] - e) & 3
            rows = pl.ds(pl.multiple_of((z * 4 + y) * B, B), B)
            up[rows, :] = s[e, :, :512]
            query[rows, :] = s[e, :, 512:640]
            key[rows, :] = s[e, :, 640:]


def unpack_b_kernel(at_ref, s0, s1, s2, s3, down, mixed, value, norm, bias):
    lane = lax.broadcasted_iota(jnp.int32, (8, 128), 1)
    for d, s in enumerate((s0, s1, s2, s3)):
        z = (at_ref[0] - d) & 3
        for p in range(2):
            e0 = (at_ref[1] - 2 * p) & 3
            e1 = (at_ref[1] - 2 * p - 1) & 3
            pair = z * 2 + p
            at = pl.ds(pl.multiple_of(pair * 128, 128), 128)

            def get(k):
                return jnp.concatenate([s[e0, k * B : k * B + B, :], s[e1, k * B : k * B + B, :]], axis=0)

            for k in range(4):
                down[k * 128 : k * 128 + 128, at] = get(k).T
            mixed[:, at] = get(4).T
            value[at, :] = get(5)
            last = jnp.where(
                lane < B, s[e0, 6 * B :, :].astype(jnp.float32), s[e1, 6 * B :, :].astype(jnp.float32)
            )
            norm[pl.ds(pair, 1), :] = last[0:1]
            bias[pl.ds(pair, 1), :] = last[1:2]


def unpack(kernel, name, place, stacks, shapes):
    return pl.pallas_call(
        kernel,
        in_specs=[pl.BlockSpec(memory_space=pltpu.SMEM)] + [pl.BlockSpec(memory_space=pltpu.VMEM)] * 4,
        out_shape=tuple(jax.ShapeDtypeStruct(*s) for s in shapes),
        name=name,
    )(place, *stacks)


def local(*args):
    slopes, params, states = args[:8], args[8:16], args[16:24]
    f16, f32, bf16 = jnp.float16, jnp.float32, jnp.bfloat16
    at = lax.axis_index("replica").astype(jnp.int32)
    zi, yi = at >> 2, at & 3
    place = jnp.stack([zi, yi])

    def inner(xs):
        up, down, query, key, value, mixed, norm, bias = xs
        return up, query, key, down.T, mixed.T, value, norm[None], bias[None]

    params, states = inner(params), inner(states)

    grid_a = [s[0].reshape(4, 4, B, -1) for s in (slopes[0], slopes[2], slopes[3])]

    def chunk_a(d):
        one = [lax.dynamic_index_in_dim(s, (yi + d) & 3, 1, keepdims=False) for s in grid_a]
        return jnp.concatenate(one, axis=2) * SCALE

    got_a = [send(chunk_a(d).astype(f16), "y", d) for d in (2, 1, 3)]
    packed = pack(place, slopes[1], slopes[5], slopes[4], slopes[6], slopes[7])
    got_b = [send(packed[d].astype(f16), "z", d) for d in (2, 1, 3)]

    def four_a(e):
        def pick(x):
            return lax.dynamic_index_in_dim(x, (zi + e) & 3, 0, keepdims=False).astype(f32)

        return (pick(chunk_a(0)) + sum(pick(g) for g in got_a)) * 0.25

    def four_b(e):
        return (packed[0, e] + sum(g[e].astype(f32) for g in got_b)) * 0.25

    then_a = [send(four_a(e).astype(f16), "z", e) for e in (2, 1, 3)]
    sum_a = four_a(0) + sum(g.astype(f32) for g in then_a)
    then_b = [send(four_b(e).astype(f16), "y", e) for e in (2, 1, 3)]
    sum_b = four_b(0) + sum(g.astype(f32) for g in then_b)

    part = norms(lax.axis_size("model"), sum_a, sum_b, *params[:6])
    parts = lax.all_to_all(part, "model", 0, 0, tiled=True)
    nexts, news, half_a, half_b = update(parts, sum_a, sum_b, params, states)

    own_a = jnp.stack([half_a] + [send(half_a, "z", d) for d in (1, 2, 3)])
    own_b = jnp.stack([half_b] + [send(half_b, "y", d) for d in (1, 2, 3)])
    all_a = [own_a] + [send(own_a, "y", d) for d in (1, 2, 3)]
    all_b = [own_b] + [send(own_b, "z", d) for d in (1, 2, 3)]
    up, query, key = unpack(
        unpack_a_kernel, "unpack_a", place, all_a, (((1024, 512), bf16), ((1024, 128), bf16), ((1024, 128), bf16))
    )
    down, mixed, value, norm, bias = unpack(
        unpack_b_kernel,
        "unpack_b",
        place,
        all_b,
        (((512, 1024), bf16), ((128, 1024), bf16), ((1024, 128), bf16), ((8, 128), f32), ((8, 128), f32)),
    )
    norm, bias = norm.reshape(1024).astype(bf16), bias.reshape(1024).astype(bf16)

    def outer(xs):
        up, query, key, down, mixed, value, norm, bias = xs
        return up, down.T, query, key, value, mixed.T, norm[0], bias[0]

    return (up, down, query, key, value, mixed, norm, bias, *outer(nexts), *outer(news))


def solution(mesh):
    cut = [P("replica", "model"), P("model", "replica")] + [P("replica", "model")] * 3
    cut += [P("model", "replica"), P("replica"), P("replica")]
    slope = [P("replica", None, "model"), P("replica", "model", None)] + [P("replica", None, "model")] * 3
    slope += [P("replica", "model", None), P("replica", None), P("replica", None)]
    half = [P(None, "model"), P("model", None)] + [P(None, "model")] * 3 + [P("model", None), P(), P()]
    return jax.shard_map(
        local,
        mesh=mesh,
        in_specs=(*slope, *cut, *cut),
        out_specs=(*half, *cut, *cut),
        check_vma=False,
    )
```

```python
import jax
import jax.numpy as jnp
from jax import lax
from jax.experimental import pallas as pl
from jax.experimental.pallas import tpu as pltpu
from jax.sharding import PartitionSpec as P


learn_rate = 0.025
hold_rate = 0.7

B = 64
TB = 6 * B + 8
SCALE = 8192.0
SCALE_VEC = 4096.0
A_COLS = ((0, 4), (4, 1), (5, 1))
B_COLS = ((0, 4), (4, 1), (5, 1))


ORDER = (0, 2, 1, 3)


def place_of(d):
    return jnp.where(d == 1, 2, jnp.where(d == 2, 1, d))


def shift(dz, dy):
    return [(z * 4 + y, (z + dz) % 4 * 4 + (y + dy) % 4) for z in range(4) for y in range(4)]


def along(axis, d):
    return shift(d, 0) if axis == "z" else shift(0, d)


def send(x, axis, d):
    return lax.ppermute(x, "replica", along(axis, d))


def in_vmem(x):
    return pltpu.with_memory_space_constraint(x, pltpu.VMEM)


VM = pl.BlockSpec(memory_space=pltpu.VMEM)
SM = pl.BlockSpec(memory_space=pltpu.SMEM)
HB = pl.BlockSpec(memory_space=pltpu.HBM)


def pack_kernel(at_ref, up, query, key, down, mixed, value, norm, bias, out_a, out_b, sems):
    zi, yi = at_ref[0], at_ref[1]
    copies = []

    def copy(source, target):
        copies.append(pltpu.make_async_copy(source, target, sems.at[len(copies)]))
        copies[-1].start()

    for d in (2, 1, 3, 0):
        y, z = (yi + d) & 3, (zi + d) & 3
        for e in range(4):
            rows = pl.ds(pl.multiple_of((((zi + e) & 3) * 4 + y) * B, B), B)
            copy(up.at[0, rows], out_a.at[d, e, :, pl.ds(0, 512)])
            copy(query.at[0, rows], out_a.at[d, e, :, pl.ds(512, 128)])
            copy(key.at[0, rows], out_a.at[d, e, :, pl.ds(640, 128)])
        columns = pl.ds(pl.multiple_of(z * 256, 256), 256)
        copy(down.at[0, :, columns], out_b.at[d, pl.ds(0, 512)])
        copy(mixed.at[0, :, columns], out_b.at[d, pl.ds(512, 128)])
        for h in range(2):
            rows = pl.ds(pl.multiple_of(z * 256 + h * 128, 128), 128)
            copy(value.at[0, rows], out_b.at[d, pl.ds(640, 128), pl.ds(h * 128, 128)])
        n = jnp.broadcast_to(norm[0:1, columns] * 0.5, (8, 256))
        b = jnp.broadcast_to(bias[0:1, columns] * 0.5, (8, 256))
        row = lax.broadcasted_iota(jnp.int32, (8, 256), 0)
        out_b[d, 768:, :] = jnp.where(row == 0, n, jnp.where(row == 1, b, 0.0))
    for c in copies:
        c.wait()


def pack(place, *slopes):
    return pl.pallas_call(
        pack_kernel,
        in_specs=[SM] + [HB] * 6 + [VM] * 2,
        out_specs=(VM, VM),
        out_shape=(pltpu.VMEM((4, 4, B, 768), jnp.float32), pltpu.VMEM((4, 776, 256), jnp.float32)),
        scratch_shapes=[pltpu.SemaphoreType.DMA((64,))],
        compiler_params=pltpu.CompilerParams(vmem_limit_bytes=24 << 20),
        name="pack",
    )(place, *[pltpu.with_memory_space_constraint(x, pltpu.HBM) for x in slopes[:6]], *[in_vmem(x) for x in slopes[6:]])


def turn_kernel(at_ref, x, out):
    for p in range(2):
        lanes = slice(p * 128, p * 128 + 128)
        tiles = [x[k * 128 : k * 128 + 128, lanes].T for k in range(5)]
        tiles.append(x[640:768, lanes])
        for j in range(2):
            e = (2 * p + j - at_ref[1]) & 3
            for k, tile in enumerate(tiles):
                out[pl.ds(e, 1), k * B : k * B + B, :] = tile[None, j * B : j * B + B]
            last = x[768:776, lanes]
            out[pl.ds(e, 1), 6 * B :, :] = (last if j == 0 else pltpu.roll(last, 64, 1))[None]


def turn(place, x):
    return pl.pallas_call(
        turn_kernel,
        in_specs=[SM, VM],
        out_specs=VM,
        out_shape=pltpu.VMEM((4, TB, 128), jnp.float32),
        compiler_params=pltpu.CompilerParams(vmem_limit_bytes=24 << 20),
        name="turn",
    )(place, in_vmem(x))


def norms_kernel(sum_a, sum_b, p_up, p_query, p_key, p_down, p_mixed, p_value, part):
    lane = lax.broadcasted_iota(jnp.int32, (B, 128), 1)
    params = (p_up, p_query, p_key, p_down, p_mixed, p_value)
    table = jnp.zeros((B, 128), jnp.float32)
    for m, (col, n) in enumerate(A_COLS + B_COLS):
        squares = jnp.zeros((B, 128), jnp.float32)
        own = jnp.zeros((B, 128), jnp.float32)
        for k in range(n):
            c = col + k
            x = sum_a[:, c * 128 : c * 128 + 128] if m < 3 else sum_b[c * B : c * B + B, :]
            x = x * (1.0 / SCALE)
            squares = squares + x * x
            p = params[m][:, k * 128 : k * 128 + 128]
            own = own + p * p
        s = jnp.sum(squares, axis=1, keepdims=True)
        o = jnp.sum(own, axis=1, keepdims=True)
        table = jnp.where(lane == m, o, jnp.where(lane == 8 + m, s, table))
    table = jnp.concatenate([table, jnp.zeros((128 - B, 128), jnp.float32)], axis=0)
    table = table.T[:16, :]
    for r in range(part.shape[0]):
        part[r] = table


def norms(copies, sum_a, sum_b, *params):
    return pl.pallas_call(
        norms_kernel,
        in_specs=[VM] * 8,
        out_specs=VM,
        out_shape=pltpu.VMEM((copies, 16, 128), jnp.float32),
        compiler_params=pltpu.CompilerParams(vmem_limit_bytes=24 << 20),
        name="norms",
    )(in_vmem(sum_a), in_vmem(sum_b), *params)


def steps(parts, sum_a, sum_b, params, states, store, store_half):
    sums = parts[0]
    for d in range(1, parts.shape[0]):
        sums = sums + parts[d]
    ratio = jnp.sqrt(sums[:8]) * lax.rsqrt(sums[8:16] + 1e-06)
    ratio = jnp.concatenate([ratio, jnp.zeros((120, 128), jnp.float32)], axis=0).T[:B, :]

    def step(m, param, state):
        new = hold_rate * state + (1.0 - hold_rate) * m * m
        return param - learn_rate * m * lax.rsqrt(new + 1e-06), new

    for i, (col, n) in enumerate(A_COLS + B_COLS):
        r = ratio[:, i : i + 1]
        for k in range(n):
            c = col + k
            x = sum_a[:, c * 128 : c * 128 + 128] if i < 3 else sum_b[c * B : c * B + B, :]
            lanes = slice(k * 128, k * 128 + 128)
            nxt, new = step(x * (1.0 / SCALE) * r, params[i][:, lanes], states[i][:, lanes])
            store(i, lanes, nxt, new)
            store_half(i, c, nxt)
    both = []
    for j in range(2):
        m = sum_b[6 * B + j : 6 * B + j + 1, :B] * (1.0 / SCALE_VEC)
        nxt, new = step(m, params[6 + j][...], states[6 + j][...])
        store(6 + j, slice(None), nxt, new)
        both.append(jnp.concatenate([nxt, nxt], axis=1))
    row = lax.broadcasted_iota(jnp.int32, (8, 128), 0)
    n = jnp.broadcast_to(both[0], (8, 128))
    b = jnp.broadcast_to(both[1], (8, 128))
    store_half(6, 6, jnp.where(row == 0, n, jnp.where(row == 1, b, 0.0)))


def halves_kernel(parts, sum_a, sum_b, *refs):
    half_a, half_b = refs[16:]

    def store_half(i, c, nxt):
        if i < 3:
            half_a[:, c * 128 : c * 128 + 128] = nxt.astype(jnp.bfloat16)
        else:
            half_b[c * B : c * B + nxt.shape[0], :] = nxt.astype(jnp.bfloat16)

    steps(parts, sum_a, sum_b, refs[:8], refs[8:16], lambda *_: None, store_half)


def halves(parts, sum_a, sum_b, params, states):
    return pl.pallas_call(
        halves_kernel,
        in_specs=[VM] * 19,
        out_specs=(VM, VM),
        out_shape=(pltpu.VMEM((B, 768), jnp.bfloat16), pltpu.VMEM((TB, 128), jnp.bfloat16)),
        compiler_params=pltpu.CompilerParams(vmem_limit_bytes=24 << 20),
        name="halves",
    )(in_vmem(parts), in_vmem(sum_a), in_vmem(sum_b), *params, *states)


def update_kernel(parts, sum_a, sum_b, *refs):
    nexts, news = refs[16:24], refs[24:32]

    def store(i, lanes, nxt, new):
        nexts[i][:, lanes] = nxt
        news[i][:, lanes] = new

    steps(parts, sum_a, sum_b, refs[:8], refs[8:16], store, lambda *_: None)


def update(parts, sum_a, sum_b, params, states):
    shapes = [jax.ShapeDtypeStruct(p.shape, jnp.float32) for p in params]
    out = pl.pallas_call(
        update_kernel,
        in_specs=[VM] * 19,
        out_shape=(*shapes, *shapes),
        compiler_params=pltpu.CompilerParams(vmem_limit_bytes=24 << 20),
        name="update",
    )(in_vmem(parts), in_vmem(sum_a), in_vmem(sum_b), *params, *states)
    return out[:8], out[8:]


def unpack_a_kernel(at_ref, s0, s1, s2, s3, up, query, key, sems):
    copies = []
    for d, s in zip(ORDER, (s0, s1, s2, s3)):
        y = (at_ref[1] - d) & 3
        for e in range(4):
            z = (at_ref[0] - ORDER[e]) & 3
            rows = pl.ds(pl.multiple_of((z * 4 + y) * B, B), B)
            for target, lanes in ((up, (0, 512)), (query, (512, 128)), (key, (640, 128))):
                copies.append(
                    pltpu.make_async_copy(s.at[e, :, pl.ds(*lanes)], target.at[rows], sems.at[len(copies)])
                )
                copies[-1].start()
    for c in copies:
        c.wait()


def unpack_a(place, stacks):
    bf16 = jnp.bfloat16
    return pl.pallas_call(
        unpack_a_kernel,
        in_specs=[SM] + [VM] * 4,
        out_specs=(HB,) * 3,
        out_shape=tuple(jax.ShapeDtypeStruct((1024, n), bf16) for n in (512, 128, 128)),
        scratch_shapes=[pltpu.SemaphoreType.DMA((48,))],
        compiler_params=pltpu.CompilerParams(vmem_limit_bytes=24 << 20),
        name="unpack_a",
    )(place, *[in_vmem(s) for s in stacks])


def unpack_b_kernel(at_ref, s0, s1, s2, s3, down, mixed, value, vectors):
    lane = lax.broadcasted_iota(jnp.int32, (8, 128), 1)
    for d, s in zip(ORDER, (s0, s1, s2, s3)):
        z = (at_ref[0] - d) & 3
        for p in range(2):
            e0 = place_of((at_ref[1] - 2 * p) & 3)
            e1 = place_of((at_ref[1] - 2 * p - 1) & 3)
            pair = z * 2 + p
            at = pl.ds(pl.multiple_of(pair * 128, 128), 128)

            def get(k):
                return jnp.concatenate([s[e0, k * B : k * B + B, :], s[e1, k * B : k * B + B, :]], axis=0)

            for k in range(4):
                down[k * 128 : k * 128 + 128, at] = get(k).T
            mixed[:, at] = get(4).T
            value[at, :] = get(5)
            last = jnp.where(
                lane < B, s[e0, 6 * B :, :].astype(jnp.float32), s[e1, 6 * B :, :].astype(jnp.float32)
            )
            vectors[pl.ds(pair, 1), :] = last[0:1]
            vectors[pl.ds(8 + pair, 1), :] = last[1:2]


def unpack_b(place, stacks):
    bf16 = jnp.bfloat16
    return pl.pallas_call(
        unpack_b_kernel,
        in_specs=[SM] + [VM] * 4,
        out_shape=(
            jax.ShapeDtypeStruct((512, 1024), bf16),
            jax.ShapeDtypeStruct((128, 1024), bf16),
            jax.ShapeDtypeStruct((1024, 128), bf16),
            jax.ShapeDtypeStruct((16, 128), jnp.float32),
        ),
        compiler_params=pltpu.CompilerParams(vmem_limit_bytes=24 << 20),
        name="unpack_b",
    )(place, *[in_vmem(s) for s in stacks])


def local(*args):
    slopes, params, states = args[:8], args[8:16], args[16:24]
    f16, f32, bf16 = jnp.float16, jnp.float32, jnp.bfloat16
    at = lax.axis_index("replica").astype(jnp.int32)
    zi, yi = at >> 2, at & 3
    place = jnp.stack([zi, yi])

    def inner(xs):
        up, down, query, key, value, mixed, norm, bias = xs
        return up, query, key, down.T, mixed.T, value, norm[None], bias[None]

    params, states = inner(params), inner(states)

    near = [in_vmem(x) for x in params], [in_vmem(x) for x in states]

    packed_a, packed_b = pack(place, slopes[0], slopes[2], slopes[3], slopes[1], slopes[5], slopes[4], *slopes[6:])
    got_a, got_b = [], []
    for d in (2, 1, 3):
        got_a.append(send((packed_a[d] * SCALE).astype(f16), "y", d))
        got_b.append(send((packed_b[d] * SCALE).astype(f16), "z", d))

    four_a = (packed_a[0] * SCALE + sum(g.astype(f32) for g in got_a)) * 0.25
    own_a, *out_a = lax.optimization_barrier((four_a[0], *[four_a[e].astype(f16) for e in (2, 1, 3)]))
    four_b = turn(place, (packed_b[0] * SCALE + sum(g.astype(f32) for g in got_b)) * 0.25)
    sum_a = own_a + sum(send(x, "z", e).astype(f32) for x, e in zip(out_a, (2, 1, 3)))
    sum_b = four_b[0] + sum(send(four_b[e].astype(f16), "y", e).astype(f32) for e in (2, 1, 3))

    part = norms(lax.axis_size("model"), sum_a, sum_b, *near[0][:6])
    parts = lax.all_to_all(part, "model", 0, 0, tiled=True)
    half_a, half_b = halves(parts, sum_a, sum_b, *near)

    own_a = jnp.stack([half_a] + [send(half_a, "z", d) for d in (2, 1, 3)])
    own_b = jnp.stack([half_b] + [send(half_b, "y", d) for d in (2, 1, 3)])
    all_a = [own_a] + [send(own_a, "y", d) for d in (2, 1, 3)]
    all_b = [own_b] + [send(own_b, "z", d) for d in (2, 1, 3)]
    late = lax.optimization_barrier((parts, own_a, own_b))[0]
    nexts, news = update(late, sum_a, sum_b, *near)
    up, query, key = unpack_a(place, all_a)
    down, mixed, value, vectors = unpack_b(place, all_b)
    vectors = vectors.astype(bf16)
    norm, bias = vectors[:8].reshape(1024), vectors[8:].reshape(1024)

    def outer(xs):
        up, query, key, down, mixed, value, norm, bias = xs
        return up, down.T, query, key, value, mixed.T, norm[0], bias[0]

    return (up, down, query, key, value, mixed, norm, bias, *outer(nexts), *outer(news))


def solution(mesh):
    cut = [P("replica", "model"), P("model", "replica")] + [P("replica", "model")] * 3
    cut += [P("model", "replica"), P("replica"), P("replica")]
    slope = [P("replica", None, "model"), P("replica", "model", None)] + [P("replica", None, "model")] * 3
    slope += [P("replica", "model", None), P("replica", None), P("replica", None)]
    half = [P(None, "model"), P("model", None)] + [P(None, "model")] * 3 + [P("model", None), P(), P()]
    return jax.shard_map(
        local,
        mesh=mesh,
        in_specs=(*slope, *cut, *cut),
        out_specs=(*half, *cut, *cut),
        check_vma=False,
    )
```

```python
import jax
import jax.numpy as jnp
from jax import lax
from jax.experimental import pallas as pl
from jax.experimental.pallas import tpu as pltpu
from jax.sharding import PartitionSpec as P


learn_rate = 0.025
hold_rate = 0.7

B = 64
T = 12 * B + 8
COLS = ((0, 4), (4, 1), (5, 1), (6, 1), (7, 4), (11, 1))
AT_VALUE = 4 * 3 * B
AT_DOWN = AT_VALUE + 2 * B
AT_MIXED = AT_DOWN + 512
AT_LAST = AT_MIXED + 128
ROWS = AT_LAST + 8
SCALE = 8192.0
SCALE_VEC = 4096.0
ORDER = (0, 2, 1, 3)


def vmem(x):
    return pltpu.with_memory_space_constraint(x, pltpu.VMEM)


def hbm(x):
    return pltpu.with_memory_space_constraint(x, pltpu.HBM)


VM = pl.BlockSpec(memory_space=pltpu.VMEM)
SM = pl.BlockSpec(memory_space=pltpu.SMEM)
HB = pl.BlockSpec(memory_space=pltpu.HBM)
PARAMS = pltpu.CompilerParams(vmem_limit_bytes=24 << 20)


def send(x, stage, d):
    pairs = []
    for z in range(4):
        for y in range(4):
            for m in range(8):
                along_y = (m % 2 == 0) == (stage == 0)
                to = (z * 4 + (y + d) % 4) if along_y else ((z + d) % 4 * 4 + y)
                pairs.append(((z * 4 + y) * 8 + m, to * 8 + m))
    return lax.ppermute(x, ("replica", "model"), pairs)


def block_of(at_ref, f, s):
    c = at_ref[2]
    return f * (1 + 3 * c) + s * (4 - 3 * c)


def pack(place, slopes, distances):
    n = len(distances)

    def kernel(at_ref, up, query, key, value, down, mixed, norm, bias, out, down_s, mixed_s, norm_s, bias_s, sems):
        fi, si, c = at_ref[0], at_ref[1], at_ref[2]
        copies = []

        def copy(source, target):
            copies.append(pltpu.make_async_copy(source, target, sems.at[len(copies)]))
            copies[-1].start()

        copy(down.at[0], down_s)
        copy(mixed.at[0], mixed_s)
        copy(norm, norm_s)
        copy(bias, bias_s)
        for o, d in enumerate(distances):
            for e in range(4):
                r = block_of(at_ref, (fi + d) & 3, (si + e) & 3)
                rows = pl.ds(pl.multiple_of(r * B, B), B)
                for h in range(2):
                    copy(up.at[0, rows, pl.ds(h * 256, 256)], out.at[o, pl.ds(e * 192 + h * B, B)])
                pair = pl.ds(e * 192 + 128, B)
                copy(query.at[0, rows], out.at[o, pair, pl.ds(0, 128)])
                copy(key.at[0, rows], out.at[o, pair, pl.ds(128, 128)])
                copy(value.at[0, rows], out.at[o, pl.ds(AT_VALUE + e // 2 * B, B), pl.ds(e % 2 * 128, 128)])
        for k in range(4):
            copies[k].wait()
        lane = lax.broadcasted_iota(jnp.int32, (B, 128), 1)
        for o, d in enumerate(distances):
            f = (fi + d) & 3
            turn_l = jnp.where(c == 0, (f & 1) * 64, 0)
            turn_r = jnp.where(c == 0, 64 - (f & 1) * 64, 0)
            for h in range(2):
                t_l = jnp.where(c == 0, h * 4 + (f >> 1), f * 2 + h)
                t_r = jnp.where(c == 0, h * 4 + 2 + (f >> 1), f * 2 + h)
                at_l = pl.ds(pl.multiple_of(t_l * 128, 128), 128)
                at_r = pl.ds(pl.multiple_of(t_r * 128, 128), 128)
                to = slice(h * 128, h * 128 + 128)

                def both(left, right):
                    left, right = pltpu.roll(left, turn_l, 1), pltpu.roll(right, turn_r, 1)
                    return jnp.where(lane[: left.shape[0]] < 64, left, right)

                for k in range(8):
                    rows = slice(k * B, k * B + B)
                    out[o, AT_DOWN + k * B : AT_DOWN + k * B + B, to] = both(down_s[rows, at_l], down_s[rows, at_r])
                for k in range(2):
                    rows = slice(k * B, k * B + B)
                    out[o, AT_MIXED + k * B : AT_MIXED + k * B + B, to] = both(mixed_s[rows, at_l], mixed_s[rows, at_r])
                row = lax.broadcasted_iota(jnp.int32, (8, 128), 0)

                def last(at):
                    n = jnp.broadcast_to(norm_s[0:1, at] * 0.5, (8, 128))
                    b = jnp.broadcast_to(bias_s[0:1, at] * 0.5, (8, 128))
                    return jnp.where(row == 0, n, jnp.where(row == 1, b, 0.0))

                out[o, AT_LAST:ROWS, to] = both(last(at_l), last(at_r))
        for k in range(4, len(copies)):
            copies[k].wait()

    f32 = jnp.float32
    return pl.pallas_call(
        kernel,
        in_specs=[SM] + [HB] * 8,
        out_specs=VM,
        out_shape=pltpu.VMEM((n, ROWS, 256), f32),
        scratch_shapes=[
            pltpu.VMEM((512, 1024), f32),
            pltpu.VMEM((128, 1024), f32),
            pltpu.VMEM((1, 1024), f32),
            pltpu.VMEM((1, 1024), f32),
            pltpu.SemaphoreType.DMA((4 + 20 * n,)),
        ],
        compiler_params=PARAMS,
        name=f"pack_{n}",
    )(place, *[hbm(x) for x in slopes])


def turn_kernel(at_ref, x, out):
    for e in range(4):
        for k in range(6):
            at = e * 192 + k // 2 * B
            out[e, k * B : k * B + B, :] = x[at : at + B, k % 2 * 128 : k % 2 * 128 + 128]
        at = AT_VALUE + e // 2 * B
        out[e, 6 * B : 7 * B, :] = x[at : at + B, e % 2 * 128 : e % 2 * 128 + 128]
    for h in range(2):
        lanes = slice(h * 128, h * 128 + 128)
        tiles = [x[AT_DOWN + k * 128 : AT_DOWN + k * 128 + 128, lanes].T for k in range(5)]
        last = x[AT_LAST:ROWS, lanes]
        for j in range(2):
            e = (2 * h + j - at_ref[1]) & 3
            for k, tile in enumerate(tiles):
                out[pl.ds(e, 1), (7 + k) * B : (8 + k) * B, :] = tile[None, j * B : j * B + B]
            out[pl.ds(e, 1), 12 * B :, :] = (last if j == 0 else pltpu.roll(last, 64, 1))[None]


def turn(place, x):
    return pl.pallas_call(
        turn_kernel,
        in_specs=[SM, VM],
        out_specs=VM,
        out_shape=pltpu.VMEM((4, T, 128), jnp.float32),
        compiler_params=PARAMS,
        name="turn",
    )(place, vmem(x))


def norms_kernel(total, p_up, p_query, p_key, p_value, p_down, p_mixed, part):
    lane = lax.broadcasted_iota(jnp.int32, (B, 128), 1)
    params = (p_up, p_query, p_key, p_value, p_down, p_mixed)
    table = jnp.zeros((B, 128), jnp.float32)
    for m, (col, n) in enumerate(COLS):
        squares = jnp.zeros((B, 128), jnp.float32)
        own = jnp.zeros((B, 128), jnp.float32)
        for k in range(n):
            x = total[(col + k) * B : (col + k + 1) * B, :] * (1.0 / SCALE)
            squares = squares + x * x
            p = params[m][:, k * 128 : k * 128 + 128]
            own = own + p * p
        s = jnp.sum(squares, axis=1, keepdims=True)
        o = jnp.sum(own, axis=1, keepdims=True)
        table = jnp.where(lane == m, o, jnp.where(lane == 8 + m, s, table))
    table = jnp.concatenate([table, jnp.zeros((128 - B, 128), jnp.float32)], axis=0)
    table = table.T[:16, :]
    for r in range(part.shape[0]):
        part[r] = table


def norms(copies, total, *params):
    return pl.pallas_call(
        norms_kernel,
        in_specs=[VM] * 7,
        out_specs=VM,
        out_shape=pltpu.VMEM((copies, 16, 128), jnp.float32),
        compiler_params=PARAMS,
        name="norms",
    )(vmem(total), *params)


def steps(parts, total, params, states, store, store_half):
    sums = parts[0]
    for d in range(1, parts.shape[0]):
        sums = sums + parts[d]
    ratio = jnp.sqrt(sums[:8]) * lax.rsqrt(sums[8:16] + 1e-06)
    ratio = jnp.concatenate([ratio, jnp.zeros((120, 128), jnp.float32)], axis=0).T[:B, :]

    def step(m, param, state):
        new = hold_rate * state + (1.0 - hold_rate) * m * m
        return param - learn_rate * m * lax.rsqrt(new + 1e-06), new

    for i, (col, n) in enumerate(COLS):
        r = ratio[:, i : i + 1]
        for k in range(n):
            at = (col + k) * B
            lanes = slice(k * 128, k * 128 + 128)
            m = total[at : at + B, :] * (1.0 / SCALE) * r
            nxt, new = step(m, params[i][:, lanes], states[i][:, lanes])
            store(i, lanes, nxt, new)
            store_half(at, nxt)
    both = []
    for j in range(2):
        m = total[12 * B + j : 12 * B + j + 1, :B] * (1.0 / SCALE_VEC)
        nxt, new = step(m, params[6 + j][...], states[6 + j][...])
        store(6 + j, slice(None), nxt, new)
        both.append(jnp.concatenate([nxt, nxt], axis=1))
    row = lax.broadcasted_iota(jnp.int32, (8, 128), 0)
    n = jnp.broadcast_to(both[0], (8, 128))
    b = jnp.broadcast_to(both[1], (8, 128))
    store_half(12 * B, jnp.where(row == 0, n, jnp.where(row == 1, b, 0.0)))


def halves_kernel(parts, total, *refs):
    half = refs[16]

    def store_half(at, nxt):
        half[at : at + nxt.shape[0], :] = nxt.astype(jnp.bfloat16)

    steps(parts, total, refs[:8], refs[8:16], lambda *_: None, store_half)


def halves(parts, total, params, states):
    return pl.pallas_call(
        halves_kernel,
        in_specs=[VM] * 18,
        out_specs=VM,
        out_shape=pltpu.VMEM((T, 128), jnp.bfloat16),
        compiler_params=PARAMS,
        name="halves",
    )(vmem(parts), vmem(total), *params, *states)


def update_kernel(parts, total, *refs):
    nexts, news = refs[16:24], refs[24:32]

    def store(i, lanes, nxt, new):
        nexts[i][:, lanes] = nxt
        news[i][:, lanes] = new

    steps(parts, total, refs[:8], refs[8:16], store, lambda *_: None)


def update(parts, total, params, states):
    shapes = [jax.ShapeDtypeStruct(p.shape, jnp.float32) for p in params]
    out = pl.pallas_call(
        update_kernel,
        in_specs=[VM] * 18,
        out_shape=(*shapes, *shapes),
        compiler_params=PARAMS,
        name="update",
    )(vmem(parts), vmem(total), *params, *states)
    return out[:8], out[8:]


def unpack_kernel(at_ref, s0, s1, s2, s3, up, query, key, value, down, mixed, vectors, *scratch):
    up_s, query_s, key_s, value_s, down_s, mixed_s, rest_s, sems = scratch
    for d, s in zip(ORDER, (s0, s1, s2, s3)):
        for i, e in enumerate(ORDER):
            r = block_of(at_ref, (at_ref[0] - d) & 3, (at_ref[1] - e) & 3)
            rows = pl.ds(pl.multiple_of(r * B, B), B)
            for k in range(4):
                up_s[rows, k * 128 : k * 128 + 128] = s[i, k * B : k * B + B, :]
            query_s[rows, :] = s[i, 4 * B : 5 * B, :]
            key_s[rows, :] = s[i, 5 * B : 6 * B, :]
            value_s[rows, :] = s[i, 6 * B : 7 * B, :]
            rest_s[pl.ds(r, 1)] = s[i, 7 * B :, :][None]
    pairs = ((up_s, up), (query_s, query), (key_s, key), (value_s, value), (down_s, down), (mixed_s, mixed))
    copies = [pltpu.make_async_copy(a, b, sems.at[k]) for k, (a, b) in enumerate(pairs)]
    for k in range(4):
        copies[k].start()
    lane = lax.broadcasted_iota(jnp.int32, (8, 128), 1)
    for p in range(8):
        lanes = slice(p * 128, p * 128 + 128)
        for k in range(5):
            one = [rest_s[2 * p + j, k * B : k * B + B, :] for j in range(2)]
            tile = jnp.concatenate(one, axis=0).T
            if k < 4:
                down_s[k * 128 : k * 128 + 128, lanes] = tile
            else:
                mixed_s[:, lanes] = tile
        one = [rest_s[2 * p + j, 5 * B :, :].astype(jnp.float32) for j in range(2)]
        last = jnp.where(lane < B, one[0], one[1])
        vectors[p : p + 1, :] = last[0:1]
        vectors[8 + p : 9 + p, :] = last[1:2]
    for k in range(4, 6):
        copies[k].start()
    for c in copies:
        c.wait()


def unpack(place, stacks):
    bf16 = jnp.bfloat16
    shapes = ((1024, 512), (1024, 128), (1024, 128), (1024, 128), (512, 1024), (128, 1024))
    return pl.pallas_call(
        unpack_kernel,
        in_specs=[SM] + [VM] * 4,
        out_specs=(*[HB] * 6, VM),
        out_shape=(*[jax.ShapeDtypeStruct(s, bf16) for s in shapes], pltpu.VMEM((16, 128), jnp.float32)),
        scratch_shapes=[
            *[pltpu.VMEM(s, bf16) for s in shapes],
            pltpu.VMEM((16, 5 * B + 8, 128), bf16),
            pltpu.SemaphoreType.DMA((6,)),
        ],
        compiler_params=PARAMS,
        name="unpack",
    )(place, *[vmem(s) for s in stacks])


def local(*args):
    f16, f32, bf16 = jnp.float16, jnp.float32, jnp.bfloat16
    at = lax.axis_index("replica").astype(jnp.int32)
    core = lax.axis_index("model").astype(jnp.int32) & 1
    zi, yi = at >> 2, at & 3
    place = jnp.stack([jnp.where(core == 0, yi, zi), jnp.where(core == 0, zi, yi), core])

    def inner(xs):
        up, down, query, key, value, mixed, norm, bias = xs
        return up, query, key, value, down, mixed, norm, bias

    def turned(xs):
        up, query, key, value, down, mixed, norm, bias = inner(xs)
        return [vmem(x) for x in (up, query, key, value, down.T, mixed.T, norm[None], bias[None])]

    slopes, params, states = inner(args[:8]), turned(args[8:16]), turned(args[16:24])

    packed = pack(place, slopes, ORDER[1:])
    chunks = [(packed[o] * SCALE).astype(f16) for o in range(3)]
    got = [send(x, 0, d) for x, d in zip(chunks, ORDER[1:])]
    later = lax.optimization_barrier((place, chunks))[0]
    own = pack(later, slopes, (0,))[0]
    four = turn(place, (own * SCALE + sum(g.astype(f32) for g in got)) * 0.25)
    total = four[0] + sum(send(four[e].astype(f16), 1, e).astype(f32) for e in ORDER[1:])

    part = norms(lax.axis_size("model"), total, *params[:6])
    parts = lax.all_to_all(part, "model", 0, 0, tiled=True)
    half = halves(parts, total, params, states)

    row = jnp.stack([half] + [send(half, 1, e) for e in ORDER[1:]])
    stacks = [row] + [send(row, 0, d) for d in ORDER[1:]]
    nexts, news = update(lax.optimization_barrier((parts, row))[0], total, params, states)
    up, query, key, value, down, mixed, vectors = unpack(place, stacks)
    vectors = vectors.astype(bf16)
    norm, bias = vectors[:8].reshape(1024), vectors[8:].reshape(1024)

    def outer(xs):
        up, query, key, value, down, mixed, norm, bias = xs
        return up, down.T, query, key, value, mixed.T, norm[0], bias[0]

    return (up, down, query, key, value, mixed, norm, bias, *outer(nexts), *outer(news))


def solution(mesh):
    cut = [P("replica", "model"), P("model", "replica")] + [P("replica", "model")] * 3
    cut += [P("model", "replica"), P("replica"), P("replica")]
    slope = [P("replica", None, "model"), P("replica", "model", None)] + [P("replica", None, "model")] * 3
    slope += [P("replica", "model", None), P("replica", None), P("replica", None)]
    half = [P(None, "model"), P("model", None)] + [P(None, "model")] * 3 + [P("model", None), P(), P()]
    return jax.shard_map(
        local,
        mesh=mesh,
        in_specs=(*slope, *cut, *cut),
        out_specs=(*half, *cut, *cut),
        check_vma=False,
    )
```

```python
import jax
import jax.numpy as jnp
from jax import lax
from jax.experimental import pallas as pl
from jax.experimental.pallas import tpu as pltpu
from jax.sharding import PartitionSpec as P


learn_rate = 0.025
hold_rate = 0.7

B = 64
T = 12 * B + 8
COLS = ((0, 4), (4, 1), (5, 1), (6, 1), (7, 4), (11, 1))
CUT = 4 * 3 * B
AT_VALUE = CUT
AT_DOWN = AT_VALUE + 2 * B
AT_MIXED = AT_DOWN + 512
AT_LAST = AT_MIXED + 128
ROWS = AT_LAST + 8
SCALE = 8192.0
SCALE_VEC = 4096.0
ORDER = (0, 2, 1, 3)


def vmem(x):
    return pltpu.with_memory_space_constraint(x, pltpu.VMEM)


def hbm(x):
    return pltpu.with_memory_space_constraint(x, pltpu.HBM)


VM = pl.BlockSpec(memory_space=pltpu.VMEM)
SM = pl.BlockSpec(memory_space=pltpu.SMEM)
HB = pl.BlockSpec(memory_space=pltpu.HBM)
PARAMS = pltpu.CompilerParams(vmem_limit_bytes=24 << 20)


def send(x, stage, d):
    pairs = []
    for z in range(4):
        for y in range(4):
            for m in range(8):
                along_y = (m % 2 == 0) == (stage == 0)
                to = (z * 4 + (y + d) % 4) if along_y else ((z + d) % 4 * 4 + y)
                pairs.append(((z * 4 + y) * 8 + m, to * 8 + m))
    return lax.ppermute(x, ("replica", "model"), pairs)


def block_of(at_ref, f, s):
    c = at_ref[2]
    return f * (1 + 3 * c) + s * (4 - 3 * c)


def pack(place, slopes, distances):
    n = len(distances)

    def kernel(at_ref, up, query, key, value, down, mixed, norm, bias, out, down_s, mixed_s, norm_s, bias_s, sems):
        fi, si, c = at_ref[0], at_ref[1], at_ref[2]
        copies = []

        def copy(source, target):
            copies.append(pltpu.make_async_copy(source, target, sems.at[len(copies)]))
            copies[-1].start()

        copy(down.at[0], down_s)
        copy(mixed.at[0], mixed_s)
        copy(norm, norm_s)
        copy(bias, bias_s)
        for o, d in enumerate(distances):
            for e in range(4):
                r = block_of(at_ref, (fi + d) & 3, (si + e) & 3)
                rows = pl.ds(pl.multiple_of(r * B, B), B)
                for h in range(2):
                    copy(up.at[0, rows, pl.ds(h * 256, 256)], out.at[o, pl.ds(e * 192 + h * B, B)])
                pair = pl.ds(e * 192 + 128, B)
                copy(query.at[0, rows], out.at[o, pair, pl.ds(0, 128)])
                copy(key.at[0, rows], out.at[o, pair, pl.ds(128, 128)])
                copy(value.at[0, rows], out.at[o, pl.ds(AT_VALUE + e // 2 * B, B), pl.ds(e % 2 * 128, 128)])
        for k in range(4):
            copies[k].wait()
        lane = lax.broadcasted_iota(jnp.int32, (B, 128), 1)
        for o, d in enumerate(distances):
            f = (fi + d) & 3
            turn_l = jnp.where(c == 0, (f & 1) * 64, 0)
            turn_r = jnp.where(c == 0, 64 - (f & 1) * 64, 0)
            for h in range(2):
                t_l = jnp.where(c == 0, h * 4 + (f >> 1), f * 2 + h)
                t_r = jnp.where(c == 0, h * 4 + 2 + (f >> 1), f * 2 + h)
                at_l = pl.ds(pl.multiple_of(t_l * 128, 128), 128)
                at_r = pl.ds(pl.multiple_of(t_r * 128, 128), 128)
                to = slice(h * 128, h * 128 + 128)

                def both(left, right):
                    left, right = pltpu.roll(left, turn_l, 1), pltpu.roll(right, turn_r, 1)
                    return jnp.where(lane[: left.shape[0]] < 64, left, right)

                for k in range(8):
                    rows = slice(k * B, k * B + B)
                    out[o, AT_DOWN + k * B : AT_DOWN + k * B + B, to] = both(down_s[rows, at_l], down_s[rows, at_r])
                for k in range(2):
                    rows = slice(k * B, k * B + B)
                    out[o, AT_MIXED + k * B : AT_MIXED + k * B + B, to] = both(mixed_s[rows, at_l], mixed_s[rows, at_r])
                row = lax.broadcasted_iota(jnp.int32, (8, 128), 0)

                def last(at):
                    n = jnp.broadcast_to(norm_s[0:1, at] * 0.5, (8, 128))
                    b = jnp.broadcast_to(bias_s[0:1, at] * 0.5, (8, 128))
                    return jnp.where(row == 0, n, jnp.where(row == 1, b, 0.0))

                out[o, AT_LAST:ROWS, to] = both(last(at_l), last(at_r))
        for k in range(4, len(copies)):
            copies[k].wait()

    f32 = jnp.float32
    return pl.pallas_call(
        kernel,
        in_specs=[SM] + [HB] * 8,
        out_specs=VM,
        out_shape=pltpu.VMEM((n, ROWS, 256), f32),
        scratch_shapes=[
            pltpu.VMEM((512, 1024), f32),
            pltpu.VMEM((128, 1024), f32),
            pltpu.VMEM((1, 1024), f32),
            pltpu.VMEM((1, 1024), f32),
            pltpu.SemaphoreType.DMA((4 + 20 * n,)),
        ],
        compiler_params=PARAMS,
        name=f"pack_{n}",
    )(place, *[hbm(x) for x in slopes])


def turn_kernel(at_ref, a, b, out):
    for e in range(4):
        for k in range(6):
            at = e * 192 + k // 2 * B
            out[e, k * B : k * B + B, :] = a[at : at + B, k % 2 * 128 : k % 2 * 128 + 128]
        at = AT_VALUE - CUT + e // 2 * B
        out[e, 6 * B : 7 * B, :] = b[at : at + B, e % 2 * 128 : e % 2 * 128 + 128]
    at = AT_DOWN - CUT
    for h in range(2):
        lanes = slice(h * 128, h * 128 + 128)
        tiles = [b[at + k * 128 : at + k * 128 + 128, lanes].T for k in range(5)]
        last = b[AT_LAST - CUT :, lanes]
        for j in range(2):
            e = (2 * h + j - at_ref[1]) & 3
            for k, tile in enumerate(tiles):
                out[pl.ds(e, 1), (7 + k) * B : (8 + k) * B, :] = tile[None, j * B : j * B + B]
            out[pl.ds(e, 1), 12 * B :, :] = (last if j == 0 else pltpu.roll(last, 64, 1))[None]


def turn(place, a, b):
    return pl.pallas_call(
        turn_kernel,
        in_specs=[SM, VM, VM],
        out_specs=VM,
        out_shape=pltpu.VMEM((4, T, 128), jnp.float32),
        compiler_params=PARAMS,
        name="turn",
    )(place, vmem(a), vmem(b))


def norms_kernel(total, p_up, p_query, p_key, p_value, p_down, p_mixed, part):
    lane = lax.broadcasted_iota(jnp.int32, (B, 128), 1)
    params = (p_up, p_query, p_key, p_value, p_down, p_mixed)
    table = jnp.zeros((B, 128), jnp.float32)
    for m, (col, n) in enumerate(COLS):
        squares = jnp.zeros((B, 128), jnp.float32)
        own = jnp.zeros((B, 128), jnp.float32)
        for k in range(n):
            x = total[(col + k) * B : (col + k + 1) * B, :] * (1.0 / SCALE)
            squares = squares + x * x
            p = params[m][:, k * 128 : k * 128 + 128]
            own = own + p * p
        s = jnp.sum(squares, axis=1, keepdims=True)
        o = jnp.sum(own, axis=1, keepdims=True)
        table = jnp.where(lane == m, o, jnp.where(lane == 8 + m, s, table))
    table = jnp.concatenate([table, jnp.zeros((128 - B, 128), jnp.float32)], axis=0)
    table = table.T[:16, :]
    for r in range(part.shape[0]):
        part[r] = table


def norms(copies, total, *params):
    return pl.pallas_call(
        norms_kernel,
        in_specs=[VM] * 7,
        out_specs=VM,
        out_shape=pltpu.VMEM((copies, 16, 128), jnp.float32),
        compiler_params=PARAMS,
        name="norms",
    )(vmem(total), *params)


def steps(parts, total, params, states, store, store_half):
    sums = parts[0]
    for d in range(1, parts.shape[0]):
        sums = sums + parts[d]
    ratio = jnp.sqrt(sums[:8]) * lax.rsqrt(sums[8:16] + 1e-06)
    ratio = jnp.concatenate([ratio, jnp.zeros((120, 128), jnp.float32)], axis=0).T[:B, :]

    def step(m, param, state):
        new = hold_rate * state + (1.0 - hold_rate) * m * m
        return param - learn_rate * m * lax.rsqrt(new + 1e-06), new

    for i, (col, n) in enumerate(COLS):
        r = ratio[:, i : i + 1]
        for k in range(n):
            at = (col + k) * B
            lanes = slice(k * 128, k * 128 + 128)
            m = total[at : at + B, :] * (1.0 / SCALE) * r
            nxt, new = step(m, params[i][:, lanes], states[i][:, lanes])
            store(i, lanes, nxt, new)
            store_half(at, nxt)
    both = []
    for j in range(2):
        m = total[12 * B + j : 12 * B + j + 1, :B] * (1.0 / SCALE_VEC)
        nxt, new = step(m, params[6 + j][...], states[6 + j][...])
        store(6 + j, slice(None), nxt, new)
        both.append(jnp.concatenate([nxt, nxt], axis=1))
    row = lax.broadcasted_iota(jnp.int32, (8, 128), 0)
    n = jnp.broadcast_to(both[0], (8, 128))
    b = jnp.broadcast_to(both[1], (8, 128))
    store_half(12 * B, jnp.where(row == 0, n, jnp.where(row == 1, b, 0.0)))


def halves_kernel(parts, total, *refs):
    half = refs[16]

    def store_half(at, nxt):
        half[at : at + nxt.shape[0], :] = nxt.astype(jnp.bfloat16)

    steps(parts, total, refs[:8], refs[8:16], lambda *_: None, store_half)


def halves(parts, total, params, states):
    return pl.pallas_call(
        halves_kernel,
        in_specs=[VM] * 18,
        out_specs=VM,
        out_shape=pltpu.VMEM((T, 128), jnp.bfloat16),
        compiler_params=PARAMS,
        name="halves",
    )(vmem(parts), vmem(total), *params, *states)


def update_kernel(parts, total, *refs):
    nexts, news = refs[16:24], refs[24:32]

    def store(i, lanes, nxt, new):
        nexts[i][:, lanes] = nxt
        news[i][:, lanes] = new

    steps(parts, total, refs[:8], refs[8:16], store, lambda *_: None)


def update(parts, total, params, states):
    shapes = [jax.ShapeDtypeStruct(p.shape, jnp.float32) for p in params]
    out = pl.pallas_call(
        update_kernel,
        in_specs=[VM] * 18,
        out_shape=(*shapes, *shapes),
        compiler_params=PARAMS,
        name="update",
    )(vmem(parts), vmem(total), *params, *states)
    return out[:8], out[8:]


def unpack_kernel(at_ref, *refs):
    stacks, (up, query, key, value, down, mixed, vectors, *scratch) = refs[:8], refs[8:]
    up_s, query_s, key_s, value_s, down_s, mixed_s, rest_s, sems = scratch
    for n, d in enumerate(ORDER):
        for k, e in enumerate(ORDER):
            s, i = stacks[2 * n + k // 2], k % 2
            r = block_of(at_ref, (at_ref[0] - d) & 3, (at_ref[1] - e) & 3)
            rows = pl.ds(pl.multiple_of(r * B, B), B)
            for c in range(4):
                up_s[rows, c * 128 : c * 128 + 128] = s[i, c * B : c * B + B, :]
            query_s[rows, :] = s[i, 4 * B : 5 * B, :]
            key_s[rows, :] = s[i, 5 * B : 6 * B, :]
            value_s[rows, :] = s[i, 6 * B : 7 * B, :]
            rest_s[pl.ds(r, 1)] = s[i, 7 * B :, :][None]
    pairs = ((up_s, up), (query_s, query), (key_s, key), (value_s, value), (down_s, down), (mixed_s, mixed))
    copies = [pltpu.make_async_copy(a, b, sems.at[k]) for k, (a, b) in enumerate(pairs)]
    for k in range(4):
        copies[k].start()
    lane = lax.broadcasted_iota(jnp.int32, (8, 128), 1)
    for p in range(8):
        lanes = slice(p * 128, p * 128 + 128)
        for k in range(5):
            one = [rest_s[2 * p + j, k * B : k * B + B, :] for j in range(2)]
            tile = jnp.concatenate(one, axis=0).T
            if k < 4:
                down_s[k * 128 : k * 128 + 128, lanes] = tile
            else:
                mixed_s[:, lanes] = tile
        one = [rest_s[2 * p + j, 5 * B :, :].astype(jnp.float32) for j in range(2)]
        last = jnp.where(lane < B, one[0], one[1])
        vectors[p : p + 1, :] = last[0:1]
        vectors[8 + p : 9 + p, :] = last[1:2]
    for k in range(4, 6):
        copies[k].start()
    for c in copies:
        c.wait()


def unpack(place, stacks):
    bf16 = jnp.bfloat16
    shapes = ((1024, 512), (1024, 128), (1024, 128), (1024, 128), (512, 1024), (128, 1024))
    return pl.pallas_call(
        unpack_kernel,
        in_specs=[SM] + [VM] * 8,
        out_specs=(*[HB] * 6, VM),
        out_shape=(*[jax.ShapeDtypeStruct(s, bf16) for s in shapes], pltpu.VMEM((16, 128), jnp.float32)),
        scratch_shapes=[
            *[pltpu.VMEM(s, bf16) for s in shapes],
            pltpu.VMEM((16, 5 * B + 8, 128), bf16),
            pltpu.SemaphoreType.DMA((6,)),
        ],
        compiler_params=PARAMS,
        name="unpack",
    )(place, *[vmem(s) for s in stacks])


def local(*args):
    f16, f32, bf16 = jnp.float16, jnp.float32, jnp.bfloat16
    at = lax.axis_index("replica").astype(jnp.int32)
    core = lax.axis_index("model").astype(jnp.int32) & 1
    zi, yi = at >> 2, at & 3
    place = jnp.stack([jnp.where(core == 0, yi, zi), jnp.where(core == 0, zi, yi), core])

    def inner(xs):
        up, down, query, key, value, mixed, norm, bias = xs
        return up, query, key, value, down, mixed, norm, bias

    def turned(xs):
        up, query, key, value, down, mixed, norm, bias = inner(xs)
        return [vmem(x) for x in (up, query, key, value, down.T, mixed.T, norm[None], bias[None])]

    slopes, params, states = inner(args[:8]), turned(args[8:16]), turned(args[16:24])

    packed = pack(place, slopes, ORDER[1:])
    two_a, one_a, three_a = [packed[o, :CUT] * SCALE for o in range(3)]
    two_b, one_b, three_b = [packed[o, CUT:] * SCALE for o in range(3)]
    out = [x.astype(f16) for x in (two_a, two_b, one_b, three_a)]
    got = [send(x, 0, d) for x, d in zip(out, (1, 3, 1, 3))]
    later = lax.optimization_barrier((place, out))[0]
    own = pack(later, slopes, (0,))[0] * SCALE
    through = [
        send(((one_a + got[0].astype(f32)) * 0.5).astype(f16), 0, 1),
        send(((three_b + got[1].astype(f32)) * 0.5).astype(f16), 0, 3),
    ]
    four_a = (own[:CUT] + got[3].astype(f32) + 2.0 * through[0].astype(f32)) * 0.25
    four_b = (own[CUT:] + got[2].astype(f32) + 2.0 * through[1].astype(f32)) * 0.25
    four = turn(place, four_a, four_b)
    total = four[0] + sum(send(four[e].astype(f16), 1, e).astype(f32) for e in ORDER[1:])

    part = norms(lax.axis_size("model"), total, *params[:6])
    parts = lax.all_to_all(part, "model", 0, 0, tiled=True)
    half = halves(parts, total, params, states)

    row = [half] + [send(half, 1, e) for e in ORDER[1:]]
    own_a, own_b = jnp.stack(row[:2]), jnp.stack(row[2:])
    one_a, three_a = send(own_a, 0, 1), send(own_a, 0, 3)
    three_b, one_b = send(own_b, 0, 3), send(own_b, 0, 1)
    two_a, two_b = send(one_a, 0, 1), send(three_b, 0, 3)
    stacks = [own_a, own_b, two_a, two_b, one_a, one_b, three_a, three_b]
    nexts, news = update(lax.optimization_barrier((parts, own_a, own_b))[0], total, params, states)
    up, query, key, value, down, mixed, vectors = unpack(place, stacks)
    vectors = vectors.astype(bf16)
    norm, bias = vectors[:8].reshape(1024), vectors[8:].reshape(1024)

    def outer(xs):
        up, query, key, value, down, mixed, norm, bias = xs
        return up, down.T, query, key, value, mixed.T, norm[0], bias[0]

    return (up, down, query, key, value, mixed, norm, bias, *outer(nexts), *outer(news))


def solution(mesh):
    cut = [P("replica", "model"), P("model", "replica")] + [P("replica", "model")] * 3
    cut += [P("model", "replica"), P("replica"), P("replica")]
    slope = [P("replica", None, "model"), P("replica", "model", None)] + [P("replica", None, "model")] * 3
    slope += [P("replica", "model", None), P("replica", None), P("replica", None)]
    half = [P(None, "model"), P("model", None)] + [P(None, "model")] * 3 + [P("model", None), P(), P()]
    return jax.shard_map(
        local,
        mesh=mesh,
        in_specs=(*slope, *cut, *cut),
        out_specs=(*half, *cut, *cut),
        check_vma=False,
    )
```

```python
import jax
import jax.numpy as jnp
from jax import lax
from jax.experimental import pallas as pl
from jax.experimental.pallas import tpu as pltpu
from jax.sharding import PartitionSpec as P


learn_rate = 0.025
hold_rate = 0.7

B = 64
T = 12 * B + 8
COLS = ((0, 4), (4, 1), (5, 1), (6, 1), (7, 4), (11, 1))
CUT = 4 * 3 * B
AT_VALUE = CUT
AT_DOWN = AT_VALUE + 2 * B
AT_MIXED = AT_DOWN + 512
AT_LAST = AT_MIXED + 128
ROWS = AT_LAST + 8
SCALE = 8192.0
SCALE_VEC = 4096.0
ORDER = (0, 2, 1, 3)
NEAR = (0, 1, 3, 2)


def vmem(x):
    return pltpu.with_memory_space_constraint(x, pltpu.VMEM)


def hbm(x):
    return pltpu.with_memory_space_constraint(x, pltpu.HBM)


VM = pl.BlockSpec(memory_space=pltpu.VMEM)
SM = pl.BlockSpec(memory_space=pltpu.SMEM)
HB = pl.BlockSpec(memory_space=pltpu.HBM)
PARAMS = pltpu.CompilerParams(vmem_limit_bytes=24 << 20)


def send(x, stage, d):
    pairs = []
    for z in range(4):
        for y in range(4):
            for m in range(8):
                along_y = (m % 2 == 0) == (stage == 0)
                to = (z * 4 + (y + d) % 4) if along_y else ((z + d) % 4 * 4 + y)
                pairs.append(((z * 4 + y) * 8 + m, to * 8 + m))
    return lax.ppermute(x, ("replica", "model"), pairs)


def block_of(at_ref, f, s):
    c = at_ref[2]
    return f * (1 + 3 * c) + s * (4 - 3 * c)


def pack(place, slopes, distances):
    n = len(distances)

    def kernel(at_ref, up, query, key, value, down, mixed, norm, bias, out_a, out_b, down_s, mixed_s, norm_s, bias_s, sems):
        fi, c = at_ref[0], at_ref[2]
        used = [0]

        def copy(source, target):
            one = pltpu.make_async_copy(source, target, sems.at[used[0]])
            used[0] += 1
            one.start()
            return one

        first = [copy(down.at[0, pl.ds(k * 128, 128)], down_s.at[pl.ds(k * 128, 128)]) for k in range(4)]
        first += [copy(mixed.at[0], mixed_s), copy(norm, norm_s), copy(bias, bias_s)]
        rest = []
        for o, d in enumerate(distances):
            f = (fi + d) & 3
            for s in range(4):
                rows = pl.ds(pl.multiple_of(block_of(at_ref, f, s) * B, B), B)
                target = out_b.at[o, pl.ds(s // 2 * B, B), pl.ds(s % 2 * 128, 128)]
                rest.append(copy(value.at[rows], target))
            ends = [
                (up, slice(0, 256), slice(0, B), slice(0, 256)),
                (up, slice(256, 512), slice(B, 2 * B), slice(0, 256)),
                (query, slice(0, 128), slice(2 * B, 3 * B), slice(0, 128)),
                (key, slice(0, 128), slice(2 * B, 3 * B), slice(128, 256)),
            ]
            for ref, lanes, rows, to in ends:
                at = used[0]
                used[0] += 1

                def one(source, ref=ref, lanes=lanes, rows=rows, to=to, at=at, o=o):
                    return pltpu.make_async_copy(source, out_a.at[o, :, rows, to], sems.at[at])

                @pl.when(c == 0)
                def _(ref=ref, lanes=lanes, one=one, f=f):
                    one(ref.at[:, f, :, lanes]).start()

                @pl.when(c != 0)
                def _(ref=ref, lanes=lanes, one=one, f=f):
                    one(ref.at[f, :, :, lanes]).start()

                rest.append(one(ref.at[0, :, :, lanes]))
        lane = lax.broadcasted_iota(jnp.int32, (B, 128), 1)
        row = lax.broadcasted_iota(jnp.int32, (8, 128), 0)

        def spread(ref, rows, to_row, make):
            for o, d in enumerate(distances):
                f = (fi + d) & 3
                turn_l = jnp.where(c == 0, (f & 1) * 64, 0)
                turn_r = jnp.where(c == 0, 64 - (f & 1) * 64, 0)
                for h in range(2):
                    t_l = jnp.where(c == 0, h * 4 + (f >> 1), f * 2 + h)
                    t_r = jnp.where(c == 0, h * 4 + 2 + (f >> 1), f * 2 + h)
                    left = make(ref, pl.ds(pl.multiple_of(t_l * 128, 128), 128))
                    right = make(ref, pl.ds(pl.multiple_of(t_r * 128, 128), 128))
                    left, right = pltpu.roll(left, turn_l, 1), pltpu.roll(right, turn_r, 1)
                    out_b[o, to_row : to_row + rows, h * 128 : h * 128 + 128] = jnp.where(lane[:rows] < 64, left, right)

        for k in range(10):
            if k < 8 and k % 2 == 0:
                first[k // 2].wait()
            if k == 8:
                for one in first[4:]:
                    one.wait()
            ref, at = (down_s, k * B) if k < 8 else (mixed_s, (k - 8) * B)
            spread(ref, B, AT_DOWN - CUT + k * B, lambda ref, lanes: ref[at : at + B, lanes])

        def last(refs, at):
            n = jnp.broadcast_to(refs[0][0:1, at] * 0.5, (8, 128))
            b = jnp.broadcast_to(refs[1][0:1, at] * 0.5, (8, 128))
            return jnp.where(row == 0, n, jnp.where(row == 1, b, 0.0))

        spread((norm_s, bias_s), 8, AT_LAST - CUT, last)
        for one in rest:
            one.wait()

    f32 = jnp.float32
    up, query, key, value, *others = slopes
    blocks = [x.reshape(4, 4, B, -1) for x in (up, query, key)]
    return pl.pallas_call(
        kernel,
        in_specs=[SM] + [HB] * 8,
        out_specs=(VM, VM),
        out_shape=(pltpu.VMEM((n, 4, 3 * B, 256), f32), pltpu.VMEM((n, ROWS - CUT, 256), f32)),
        scratch_shapes=[
            pltpu.VMEM((512, 1024), f32),
            pltpu.VMEM((128, 1024), f32),
            pltpu.VMEM((1, 1024), f32),
            pltpu.VMEM((1, 1024), f32),
            pltpu.SemaphoreType.DMA((7 + 8 * n,)),
        ],
        compiler_params=PARAMS,
    )(place, *[hbm(x) for x in (*blocks, value[0], *others)])


def turn_kernel(at_ref, a, b, out):
    for s in range(4):
        e = pl.ds((s - at_ref[1]) & 3, 1)
        for k in range(6):
            at = s * 192 + k // 2 * B
            out[e, k * B : k * B + B, :] = a[at : at + B, k % 2 * 128 : k % 2 * 128 + 128][None]
        at = s // 2 * B
        out[e, 6 * B : 7 * B, :] = b[at : at + B, s % 2 * 128 : s % 2 * 128 + 128][None]
    at = AT_DOWN - CUT
    for h in range(2):
        lanes = slice(h * 128, h * 128 + 128)
        tiles = [b[at + k * 128 : at + k * 128 + 128, lanes].T for k in range(5)]
        last = b[AT_LAST - CUT :, lanes]
        for j in range(2):
            e = (2 * h + j - at_ref[1]) & 3
            for k, tile in enumerate(tiles):
                out[pl.ds(e, 1), (7 + k) * B : (8 + k) * B, :] = tile[None, j * B : j * B + B]
            out[pl.ds(e, 1), 12 * B :, :] = (last if j == 0 else pltpu.roll(last, 64, 1))[None]


def turn(place, a, b):
    return pl.pallas_call(
        turn_kernel,
        in_specs=[SM, VM, VM],
        out_specs=VM,
        out_shape=pltpu.VMEM((4, T, 128), jnp.float32),
        compiler_params=PARAMS,
        name="turn",
    )(place, vmem(a), vmem(b))


def norms_kernel(total, p_up, p_query, p_key, p_value, p_down, p_mixed, part):
    lane = lax.broadcasted_iota(jnp.int32, (B, 128), 1)
    params = (p_up, p_query, p_key, p_value, p_down, p_mixed)
    table = jnp.zeros((B, 128), jnp.float32)
    for m, (col, n) in enumerate(COLS):
        squares = jnp.zeros((B, 128), jnp.float32)
        own = jnp.zeros((B, 128), jnp.float32)
        for k in range(n):
            x = total[(col + k) * B : (col + k + 1) * B, :] * (1.0 / SCALE)
            squares = squares + x * x
            p = params[m][:, k * 128 : k * 128 + 128]
            own = own + p * p
        s = jnp.sum(squares, axis=1, keepdims=True)
        o = jnp.sum(own, axis=1, keepdims=True)
        table = jnp.where(lane == m, o, jnp.where(lane == 8 + m, s, table))
    table = jnp.concatenate([table, jnp.zeros((128 - B, 128), jnp.float32)], axis=0)
    table = table.T[:16, :]
    for r in range(part.shape[0]):
        part[r] = table


def norms(copies, total, *params):
    return pl.pallas_call(
        norms_kernel,
        in_specs=[VM] * 7,
        out_specs=VM,
        out_shape=pltpu.VMEM((copies, 16, 128), jnp.float32),
        compiler_params=PARAMS,
        name="norms",
    )(vmem(total), *params)


def steps(parts, total, params, states, store, store_half):
    sums = parts[0]
    for d in range(1, parts.shape[0]):
        sums = sums + parts[d]
    ratio = jnp.sqrt(sums[:8]) * lax.rsqrt(sums[8:16] + 1e-06)
    ratio = jnp.concatenate([ratio, jnp.zeros((120, 128), jnp.float32)], axis=0).T[:B, :]

    def step(m, param, state):
        new = hold_rate * state + (1.0 - hold_rate) * m * m
        return param - learn_rate * m * lax.rsqrt(new + 1e-06), new

    for i, (col, n) in enumerate(COLS):
        r = ratio[:, i : i + 1]
        for k in range(n):
            at = (col + k) * B
            lanes = slice(k * 128, k * 128 + 128)
            m = total[at : at + B, :] * (1.0 / SCALE) * r
            nxt, new = step(m, params[i][:, lanes], states[i][:, lanes])
            store(i, lanes, nxt, new)
            store_half(at, nxt)
    both = []
    for j in range(2):
        m = total[12 * B + j : 12 * B + j + 1, :B] * (1.0 / SCALE_VEC)
        nxt, new = step(m, params[6 + j][...], states[6 + j][...])
        store(6 + j, slice(None), nxt, new)
        both.append(jnp.concatenate([nxt, nxt], axis=1))
    row = lax.broadcasted_iota(jnp.int32, (8, 128), 0)
    n = jnp.broadcast_to(both[0], (8, 128))
    b = jnp.broadcast_to(both[1], (8, 128))
    store_half(12 * B, jnp.where(row == 0, n, jnp.where(row == 1, b, 0.0)))


def halves_kernel(parts, total, *refs):
    half = refs[16]

    def store_half(at, nxt):
        half[at : at + nxt.shape[0], :] = nxt.astype(jnp.bfloat16)

    steps(parts, total, refs[:8], refs[8:16], lambda *_: None, store_half)


def halves(parts, total, params, states):
    return pl.pallas_call(
        halves_kernel,
        in_specs=[VM] * 18,
        out_specs=VM,
        out_shape=pltpu.VMEM((T, 128), jnp.bfloat16),
        compiler_params=PARAMS,
        name="halves",
    )(vmem(parts), vmem(total), *params, *states)


def update_kernel(parts, total, *refs):
    nexts, news = refs[16:24], refs[24:32]

    def store(i, lanes, nxt, new):
        nexts[i][:, lanes] = nxt
        news[i][:, lanes] = new

    steps(parts, total, refs[:8], refs[8:16], store, lambda *_: None)


def update(parts, total, params, states):
    shapes = [jax.ShapeDtypeStruct(p.shape, jnp.float32) for p in params]
    out = pl.pallas_call(
        update_kernel,
        in_specs=[VM] * 18,
        out_shape=(*shapes, *shapes),
        compiler_params=PARAMS,
        name="update",
    )(vmem(parts), vmem(total), *params, *states)
    return out[:8], out[8:]


def unpack_kernel(at_ref, *refs):
    stacks, (up, query, key, value, down, mixed, vectors, *scratch) = refs[:8], refs[8:]
    up_s, query_s, key_s, value_s, down_s, mixed_s, rest_s, sems = scratch
    for n, d in enumerate(ORDER):
        for k, e in enumerate(NEAR):
            s, i = stacks[2 * n + k // 2], k % 2
            r = block_of(at_ref, (at_ref[0] - d) & 3, (at_ref[1] - e) & 3)
            rows = pl.ds(pl.multiple_of(r * B, B), B)
            for c in range(4):
                up_s[rows, c * 128 : c * 128 + 128] = s[i, c * B : c * B + B, :]
            query_s[rows, :] = s[i, 4 * B : 5 * B, :]
            key_s[rows, :] = s[i, 5 * B : 6 * B, :]
            value_s[rows, :] = s[i, 6 * B : 7 * B, :]
            rest_s[pl.ds(r, 1)] = s[i, 7 * B :, :][None]
    pairs = ((up_s, up), (query_s, query), (key_s, key), (value_s, value), (down_s, down), (mixed_s, mixed))
    copies = [pltpu.make_async_copy(a, b, sems.at[k]) for k, (a, b) in enumerate(pairs)]
    for k in range(4):
        copies[k].start()
    lane = lax.broadcasted_iota(jnp.int32, (8, 128), 1)
    for p in range(8):
        lanes = slice(p * 128, p * 128 + 128)
        for k in range(5):
            one = [rest_s[2 * p + j, k * B : k * B + B, :] for j in range(2)]
            tile = jnp.concatenate(one, axis=0).T
            if k < 4:
                down_s[k * 128 : k * 128 + 128, lanes] = tile
            else:
                mixed_s[:, lanes] = tile
        one = [rest_s[2 * p + j, 5 * B :, :].astype(jnp.float32) for j in range(2)]
        last = jnp.where(lane < B, one[0], one[1])
        vectors[p : p + 1, :] = last[0:1]
        vectors[8 + p : 9 + p, :] = last[1:2]
    for k in range(4, 6):
        copies[k].start()
    for c in copies:
        c.wait()


def unpack(place, stacks):
    bf16 = jnp.bfloat16
    shapes = ((1024, 512), (1024, 128), (1024, 128), (1024, 128), (512, 1024), (128, 1024))
    return pl.pallas_call(
        unpack_kernel,
        in_specs=[SM] + [VM] * 8,
        out_specs=(*[HB] * 6, VM),
        out_shape=(*[jax.ShapeDtypeStruct(s, bf16) for s in shapes], pltpu.VMEM((16, 128), jnp.float32)),
        scratch_shapes=[
            *[pltpu.VMEM(s, bf16) for s in shapes],
            pltpu.VMEM((16, 5 * B + 8, 128), bf16),
            pltpu.SemaphoreType.DMA((6,)),
        ],
        compiler_params=PARAMS,
        name="unpack",
    )(place, *[vmem(s) for s in stacks])


def local(*args):
    f16, f32, bf16 = jnp.float16, jnp.float32, jnp.bfloat16
    at = lax.axis_index("replica").astype(jnp.int32)
    core = lax.axis_index("model").astype(jnp.int32) & 1
    zi, yi = at >> 2, at & 3
    place = jnp.stack([jnp.where(core == 0, yi, zi), jnp.where(core == 0, zi, yi), core])

    def inner(xs):
        up, down, query, key, value, mixed, norm, bias = xs
        return up, query, key, value, down, mixed, norm, bias

    def turned(xs):
        up, query, key, value, down, mixed, norm, bias = inner(xs)
        return [vmem(x) for x in (up, query, key, value, down.T, mixed.T, norm[None], bias[None])]

    slopes, params, states = inner(args[:8]), turned(args[8:16]), turned(args[16:24])

    packed_a, packed_b = pack(place, slopes, ORDER[1:])
    two_a, one_a, three_a = [packed_a[o].reshape(CUT, 256) * SCALE for o in range(3)]
    two_b, one_b, three_b = [packed_b[o] * SCALE for o in range(3)]
    out = [x.astype(f16) for x in (two_a, two_b, one_b, three_a)]
    got = [send(x, 0, d) for x, d in zip(out, (1, 3, 1, 3))]
    mid_a = ((one_a + got[0].astype(f32)) * 0.5).astype(f16)
    mid_b = ((three_b + got[1].astype(f32)) * 0.5).astype(f16)
    through = send(mid_a, 0, 1), send(mid_b, 0, 3)
    later = lax.optimization_barrier((place, mid_a, mid_b))[0]
    own_a, own_b = pack(later, slopes, (0,))
    four_a = (own_a.reshape(CUT, 256) * SCALE + got[3].astype(f32) + 2.0 * through[0].astype(f32)) * 0.25
    four_b = (own_b[0] * SCALE + got[2].astype(f32) + 2.0 * through[1].astype(f32)) * 0.25
    four = turn(place, four_a, four_b)
    total = four[0] + sum(send(four[e].astype(f16), 1, e).astype(f32) for e in ORDER[1:])

    part = norms(lax.axis_size("model"), total, *params[:6])
    parts = lax.all_to_all(part, "model", 0, 0, tiled=True)
    half = halves(parts, total, params, states)

    row = [half] + [send(half, 1, e) for e in NEAR[1:]]
    own_a, own_b = jnp.stack(row[:2]), jnp.stack(row[2:])

    def marked(x, d):
        return send(x, 0, d)

    one_a, three_a = marked(own_a, 1), marked(own_a, 3)
    three_b, one_b = marked(own_b, 3), marked(own_b, 1)
    two_a, two_b = marked(one_a, 1), marked(three_b, 3)
    stacks = [own_a, own_b, two_a, two_b, one_a, one_b, three_a, three_b]
    nexts, news = update(lax.optimization_barrier((parts, own_a, own_b))[0], total, params, states)
    up, query, key, value, down, mixed, vectors = unpack(place, stacks)
    vectors = vectors.astype(bf16)
    norm, bias = vectors[:8].reshape(1024), vectors[8:].reshape(1024)

    def outer(xs):
        up, query, key, value, down, mixed, norm, bias = xs
        return up, down.T, query, key, value, mixed.T, norm[0], bias[0]

    return (up, down, query, key, value, mixed, norm, bias, *outer(nexts), *outer(news))


def solution(mesh):
    cut = [P("replica", "model"), P("model", "replica")] + [P("replica", "model")] * 3
    cut += [P("model", "replica"), P("replica"), P("replica")]
    slope = [P("replica", None, "model"), P("replica", "model", None)] + [P("replica", None, "model")] * 3
    slope += [P("replica", "model", None), P("replica", None), P("replica", None)]
    half = [P(None, "model"), P("model", None)] + [P(None, "model")] * 3 + [P("model", None), P(), P()]
    return jax.shard_map(
        local,
        mesh=mesh,
        in_specs=(*slope, *cut, *cut),
        out_specs=(*half, *cut, *cut),
        check_vma=False,
    )
```

```python
import jax
import jax.numpy as jnp
from jax import lax
from jax.experimental import pallas as pl
from jax.experimental.pallas import tpu as pltpu
from jax.sharding import PartitionSpec as P


learn_rate = 0.025
hold_rate = 0.7

B = 64
T = 12 * B + 8
COLS = ((0, 4), (4, 1), (5, 1), (6, 1), (7, 4), (11, 1))
CUT = 4 * 3 * B
AT_VALUE = CUT
AT_DOWN = AT_VALUE + 2 * B
AT_MIXED = AT_DOWN + 512
AT_LAST = AT_MIXED + 128
ROWS = AT_LAST + 8
SCALE = 8192.0
SCALE_VEC = 4096.0
ORDER = (0, 2, 1, 3)


def vmem(x):
    return pltpu.with_memory_space_constraint(x, pltpu.VMEM)


def hbm(x):
    return pltpu.with_memory_space_constraint(x, pltpu.HBM)


VM = pl.BlockSpec(memory_space=pltpu.VMEM)
SM = pl.BlockSpec(memory_space=pltpu.SMEM)
HB = pl.BlockSpec(memory_space=pltpu.HBM)
PARAMS = pltpu.CompilerParams(vmem_limit_bytes=24 << 20)


def send(x, stage, d):
    pairs = []
    for z in range(4):
        for y in range(4):
            for m in range(8):
                along_y = (m % 2 == 0) == (stage == 0)
                to = (z * 4 + (y + d) % 4) if along_y else ((z + d) % 4 * 4 + y)
                pairs.append(((z * 4 + y) * 8 + m, to * 8 + m))
    return lax.ppermute(x, ("replica", "model"), pairs)


def marked(x, d, stage=1):
    return send(x, stage, d)


def block_of(at_ref, f, s):
    c = at_ref[2]
    return f * (1 + 3 * c) + s * (4 - 3 * c)


def pack(place, slopes, distances):
    n = len(distances)

    def kernel(at_ref, up, query, key, value, down, mixed, norm, bias, out_a, out_b, down_s, mixed_s, norm_s, bias_s, sems):
        fi, c = at_ref[0], at_ref[2]
        used = [0]

        def copy(source, target):
            one = pltpu.make_async_copy(source, target, sems.at[used[0]])
            used[0] += 1
            one.start()
            return one

        first = [copy(down.at[0, pl.ds(k * 128, 128)], down_s.at[pl.ds(k * 128, 128)]) for k in range(4)]
        first += [copy(mixed.at[0], mixed_s), copy(norm, norm_s), copy(bias, bias_s)]
        rest = []
        for o, d in enumerate(distances):
            f = (fi + d) & 3
            for s in range(4):
                rows = pl.ds(pl.multiple_of(block_of(at_ref, f, s) * B, B), B)
                target = out_b.at[o, pl.ds(s // 2 * B, B), pl.ds(s % 2 * 128, 128)]
                rest.append(copy(value.at[rows], target))
            ends = [
                (up, slice(0, 256), slice(0, B), slice(0, 256)),
                (up, slice(256, 512), slice(B, 2 * B), slice(0, 256)),
                (query, slice(0, 128), slice(2 * B, 3 * B), slice(0, 128)),
                (key, slice(0, 128), slice(2 * B, 3 * B), slice(128, 256)),
            ]
            for ref, lanes, rows, to in ends:
                at = used[0]
                used[0] += 1

                def one(source, ref=ref, lanes=lanes, rows=rows, to=to, at=at, o=o):
                    return pltpu.make_async_copy(source, out_a.at[o, :, rows, to], sems.at[at])

                @pl.when(c == 0)
                def _(ref=ref, lanes=lanes, one=one, f=f):
                    one(ref.at[:, f, :, lanes]).start()

                @pl.when(c != 0)
                def _(ref=ref, lanes=lanes, one=one, f=f):
                    one(ref.at[f, :, :, lanes]).start()

                rest.append(one(ref.at[0, :, :, lanes]))
        lane = lax.broadcasted_iota(jnp.int32, (B, 128), 1)
        row = lax.broadcasted_iota(jnp.int32, (8, 128), 0)

        def spread(ref, rows, to_row, make):
            for o, d in enumerate(distances):
                f = (fi + d) & 3
                turn_l = jnp.where(c == 0, (f & 1) * 64, 0)
                turn_r = jnp.where(c == 0, 64 - (f & 1) * 64, 0)
                for h in range(2):
                    t_l = jnp.where(c == 0, h * 4 + (f >> 1), f * 2 + h)
                    t_r = jnp.where(c == 0, h * 4 + 2 + (f >> 1), f * 2 + h)
                    left = make(ref, pl.ds(pl.multiple_of(t_l * 128, 128), 128))
                    right = make(ref, pl.ds(pl.multiple_of(t_r * 128, 128), 128))
                    left, right = pltpu.roll(left, turn_l, 1), pltpu.roll(right, turn_r, 1)
                    out_b[o, to_row : to_row + rows, h * 128 : h * 128 + 128] = jnp.where(lane[:rows] < 64, left, right)

        for k in range(10):
            if k < 8 and k % 2 == 0:
                first[k // 2].wait()
            if k == 8:
                for one in first[4:]:
                    one.wait()
            ref, at = (down_s, k * B) if k < 8 else (mixed_s, (k - 8) * B)
            spread(ref, B, AT_DOWN - CUT + k * B, lambda ref, lanes: ref[at : at + B, lanes])

        def last(refs, at):
            n = jnp.broadcast_to(refs[0][0:1, at] * 0.5, (8, 128))
            b = jnp.broadcast_to(refs[1][0:1, at] * 0.5, (8, 128))
            return jnp.where(row == 0, n, jnp.where(row == 1, b, 0.0))

        spread((norm_s, bias_s), 8, AT_LAST - CUT, last)
        for one in rest:
            one.wait()

    f32 = jnp.float32
    up, query, key, value, *others = slopes
    blocks = [x.reshape(4, 4, B, -1) for x in (up, query, key)]
    return pl.pallas_call(
        kernel,
        in_specs=[SM] + [HB] * 8,
        out_specs=(VM, VM),
        out_shape=(pltpu.VMEM((n, 4, 3 * B, 256), f32), pltpu.VMEM((n, ROWS - CUT, 256), f32)),
        scratch_shapes=[
            pltpu.VMEM((512, 1024), f32),
            pltpu.VMEM((128, 1024), f32),
            pltpu.VMEM((1, 1024), f32),
            pltpu.VMEM((1, 1024), f32),
            pltpu.SemaphoreType.DMA((7 + 8 * n,)),
        ],
        compiler_params=PARAMS,
    )(place, *[hbm(x) for x in (*blocks, value[0], *others)])


def turn_kernel(at_ref, a, b, out):
    for s in range(4):
        e = pl.ds((s - at_ref[1]) & 3, 1)
        for k in range(6):
            at = s * 192 + k // 2 * B
            out[e, k * B : k * B + B, :] = a[at : at + B, k % 2 * 128 : k % 2 * 128 + 128][None]
        at = s // 2 * B
        out[e, 6 * B : 7 * B, :] = b[at : at + B, s % 2 * 128 : s % 2 * 128 + 128][None]
    at = AT_DOWN - CUT
    for h in range(2):
        lanes = slice(h * 128, h * 128 + 128)
        tiles = [b[at + k * 128 : at + k * 128 + 128, lanes].T for k in range(5)]
        last = b[AT_LAST - CUT :, lanes]
        for j in range(2):
            e = (2 * h + j - at_ref[1]) & 3
            for k, tile in enumerate(tiles):
                out[pl.ds(e, 1), (7 + k) * B : (8 + k) * B, :] = tile[None, j * B : j * B + B]
            out[pl.ds(e, 1), 12 * B :, :] = (last if j == 0 else pltpu.roll(last, 64, 1))[None]


def turn(place, a, b):
    return pl.pallas_call(
        turn_kernel,
        in_specs=[SM, VM, VM],
        out_specs=VM,
        out_shape=pltpu.VMEM((4, T, 128), jnp.float32),
        compiler_params=PARAMS,
        name="turn",
    )(place, vmem(a), vmem(b))


def norms_kernel(total, p_up, p_query, p_key, p_value, p_down, p_mixed, part):
    lane = lax.broadcasted_iota(jnp.int32, (B, 128), 1)
    params = (p_up, p_query, p_key, p_value, p_down, p_mixed)
    table = jnp.zeros((B, 128), jnp.float32)
    for m, (col, n) in enumerate(COLS):
        squares = jnp.zeros((B, 128), jnp.float32)
        own = jnp.zeros((B, 128), jnp.float32)
        for k in range(n):
            x = total[(col + k) * B : (col + k + 1) * B, :] * (1.0 / SCALE)
            squares = squares + x * x
            p = params[m][:, k * 128 : k * 128 + 128]
            own = own + p * p
        s = jnp.sum(squares, axis=1, keepdims=True)
        o = jnp.sum(own, axis=1, keepdims=True)
        table = jnp.where(lane == m, o, jnp.where(lane == 8 + m, s, table))
    table = jnp.concatenate([table, jnp.zeros((128 - B, 128), jnp.float32)], axis=0)
    table = table.T[:16, :]
    part[...] = table


def norms(total, *params):
    return pl.pallas_call(
        norms_kernel,
        in_specs=[VM] * 7,
        out_specs=VM,
        out_shape=pltpu.VMEM((16, 128), jnp.float32),
        compiler_params=PARAMS,
        name="norms",
    )(vmem(total), *params)


def steps(parts, total, params, states, store, store_half):
    sums = parts[...]
    ratio = jnp.sqrt(sums[:8]) * lax.rsqrt(sums[8:16] + 1e-06)
    ratio = jnp.concatenate([ratio, jnp.zeros((120, 128), jnp.float32)], axis=0).T[:B, :]

    def step(m, param, state):
        new = hold_rate * state + (1.0 - hold_rate) * m * m
        return param - learn_rate * m * lax.rsqrt(new + 1e-06), new

    for i, (col, n) in enumerate(COLS):
        r = ratio[:, i : i + 1]
        for k in range(n):
            at = (col + k) * B
            lanes = slice(k * 128, k * 128 + 128)
            m = total[at : at + B, :] * (1.0 / SCALE) * r
            nxt, new = step(m, params[i][:, lanes], states[i][:, lanes])
            store(i, lanes, nxt, new)
            store_half(at, nxt)
    both = []
    for j in range(2):
        m = total[12 * B + j : 12 * B + j + 1, :B] * (1.0 / SCALE_VEC)
        nxt, new = step(m, params[6 + j][...], states[6 + j][...])
        store(6 + j, slice(None), nxt, new)
        both.append(jnp.concatenate([nxt, nxt], axis=1))
    row = lax.broadcasted_iota(jnp.int32, (8, 128), 0)
    n = jnp.broadcast_to(both[0], (8, 128))
    b = jnp.broadcast_to(both[1], (8, 128))
    store_half(12 * B, jnp.where(row == 0, n, jnp.where(row == 1, b, 0.0)))


def halves_kernel(parts, total, *refs):
    half = refs[16]

    def store_half(at, nxt):
        half[at : at + nxt.shape[0], :] = nxt.astype(jnp.bfloat16)

    steps(parts, total, refs[:8], refs[8:16], lambda *_: None, store_half)


def halves(parts, total, params, states):
    return pl.pallas_call(
        halves_kernel,
        in_specs=[VM] * 18,
        out_specs=VM,
        out_shape=pltpu.VMEM((T, 128), jnp.bfloat16),
        compiler_params=PARAMS,
        name="halves",
    )(vmem(parts), vmem(total), *params, *states)


def update_kernel(parts, total, *refs):
    nexts, news = refs[16:24], refs[24:32]

    def store(i, lanes, nxt, new):
        nexts[i][:, lanes] = nxt
        news[i][:, lanes] = new

    steps(parts, total, refs[:8], refs[8:16], store, lambda *_: None)


def update(parts, total, params, states):
    shapes = [jax.ShapeDtypeStruct(p.shape, jnp.float32) for p in params]
    out = pl.pallas_call(
        update_kernel,
        in_specs=[VM] * 18,
        out_shape=(*shapes, *shapes),
        compiler_params=PARAMS,
        name="update",
    )(vmem(parts), vmem(total), *params, *states)
    return out[:8], out[8:]


def unpack_kernel(at_ref, *refs):
    stacks, (up, query, key, value, down, mixed, vectors, *scratch) = refs[:8], refs[8:]
    up_s, query_s, key_s, value_s, down_s, mixed_s, rest_s, sems = scratch
    for n, d in enumerate(ORDER):
        for k, e in enumerate(ORDER):
            s, i = stacks[2 * n + k // 2], k % 2
            r = block_of(at_ref, (at_ref[0] - d) & 3, (at_ref[1] - e) & 3)
            rows = pl.ds(pl.multiple_of(r * B, B), B)
            for c in range(4):
                up_s[rows, c * 128 : c * 128 + 128] = s[i, c * B : c * B + B, :]
            query_s[rows, :] = s[i, 4 * B : 5 * B, :]
            key_s[rows, :] = s[i, 5 * B : 6 * B, :]
            value_s[rows, :] = s[i, 6 * B : 7 * B, :]
            rest_s[pl.ds(r, 1)] = s[i, 7 * B :, :][None]
    pairs = ((up_s, up), (query_s, query), (key_s, key), (value_s, value), (down_s, down), (mixed_s, mixed))
    copies = [pltpu.make_async_copy(a, b, sems.at[k]) for k, (a, b) in enumerate(pairs)]
    for k in range(4):
        copies[k].start()
    lane = lax.broadcasted_iota(jnp.int32, (8, 128), 1)
    for p in range(8):
        lanes = slice(p * 128, p * 128 + 128)
        for k in range(5):
            one = [rest_s[2 * p + j, k * B : k * B + B, :] for j in range(2)]
            tile = jnp.concatenate(one, axis=0).T
            if k < 4:
                down_s[k * 128 : k * 128 + 128, lanes] = tile
            else:
                mixed_s[:, lanes] = tile
        one = [rest_s[2 * p + j, 5 * B :, :].astype(jnp.float32) for j in range(2)]
        last = jnp.where(lane < B, one[0], one[1])
        vectors[p : p + 1, :] = last[0:1]
        vectors[8 + p : 9 + p, :] = last[1:2]
    for k in range(4, 6):
        copies[k].start()
    for c in copies:
        c.wait()


def unpack(place, stacks):
    bf16 = jnp.bfloat16
    shapes = ((1024, 512), (1024, 128), (1024, 128), (1024, 128), (512, 1024), (128, 1024))
    return pl.pallas_call(
        unpack_kernel,
        in_specs=[SM] + [VM] * 8,
        out_specs=(*[HB] * 6, VM),
        out_shape=(*[jax.ShapeDtypeStruct(s, bf16) for s in shapes], pltpu.VMEM((16, 128), jnp.float32)),
        scratch_shapes=[
            *[pltpu.VMEM(s, bf16) for s in shapes],
            pltpu.VMEM((16, 5 * B + 8, 128), bf16),
            pltpu.SemaphoreType.DMA((6,)),
        ],
        compiler_params=PARAMS,
        name="unpack",
    )(place, *[vmem(s) for s in stacks])


def local(*args):
    f16, f32, bf16 = jnp.float16, jnp.float32, jnp.bfloat16
    at = lax.axis_index("replica").astype(jnp.int32)
    core = lax.axis_index("model").astype(jnp.int32) & 1
    zi, yi = at >> 2, at & 3
    place = jnp.stack([jnp.where(core == 0, yi, zi), jnp.where(core == 0, zi, yi), core])

    def inner(xs):
        up, down, query, key, value, mixed, norm, bias = xs
        return up, query, key, value, down, mixed, norm, bias

    def turned(xs):
        up, query, key, value, down, mixed, norm, bias = inner(xs)
        return [vmem(x) for x in (up, query, key, value, down.T, mixed.T, norm[None], bias[None])]

    slopes, params, states = inner(args[:8]), turned(args[8:16]), turned(args[16:24])

    packed_a, packed_b = pack(place, slopes, ORDER[1:])
    two_a, one_a, three_a = [packed_a[o].reshape(CUT, 256) * SCALE for o in range(3)]
    two_b, one_b, three_b = [packed_b[o] * SCALE for o in range(3)]
    out = [x.astype(f16) for x in (two_a, two_b, one_b, three_a)]
    got = [send(x, 0, d) for x, d in zip(out, (1, 3, 1, 3))]
    mid_a = ((one_a + got[0].astype(f32)) * 0.5).astype(f16)
    mid_b = ((three_b + got[1].astype(f32)) * 0.5).astype(f16)
    through = send(mid_a, 0, 1), send(mid_b, 0, 3)
    later = lax.optimization_barrier((place, mid_a, mid_b))[0]
    own_a, own_b = pack(later, slopes, (0,))
    four_a = (own_a.reshape(CUT, 256) * SCALE + got[3].astype(f32) + 2.0 * through[0].astype(f32)) * 0.25
    four_b = (own_b[0] * SCALE + got[2].astype(f32) + 2.0 * through[1].astype(f32)) * 0.25
    four = turn(place, four_a, four_b)
    total = four[0] + sum(marked(four[e].astype(f16), e).astype(f32) for e in ORDER[1:])

    parts = norms(total, *params[:6])
    for partner in (lambda m: m ^ 1, lambda m: m ^ 2, lambda m: m ^ 6):
        parts = parts + lax.ppermute(parts, "model", [(m, partner(m)) for m in range(8)])
    half = halves(parts, total, params, states)

    row = [half] + [marked(half, e) for e in ORDER[1:]]
    own_a, own_b = jnp.stack(row[:2]), jnp.stack(row[2:])
    one_a, three_a = marked(own_a, 1, 0), marked(own_a, 3, 0)
    three_b, one_b = marked(own_b, 3, 0), marked(own_b, 1, 0)
    two_a, two_b = send(one_a, 0, 1), send(three_b, 0, 3)
    stacks = [own_a, own_b, two_a, two_b, one_a, one_b, three_a, three_b]
    nexts, news = update(lax.optimization_barrier((parts, own_a, own_b))[0], total, params, states)
    up, query, key, value, down, mixed, vectors = unpack(place, stacks)
    vectors = vectors.astype(bf16)
    norm, bias = vectors[:8].reshape(1024), vectors[8:].reshape(1024)

    def outer(xs):
        up, query, key, value, down, mixed, norm, bias = xs
        return up, down.T, query, key, value, mixed.T, norm[0], bias[0]

    return (up, down, query, key, value, mixed, norm, bias, *outer(nexts), *outer(news))


def solution(mesh):
    cut = [P("replica", "model"), P("model", "replica")] + [P("replica", "model")] * 3
    cut += [P("model", "replica"), P("replica"), P("replica")]
    slope = [P("replica", None, "model"), P("replica", "model", None)] + [P("replica", None, "model")] * 3
    slope += [P("replica", "model", None), P("replica", None), P("replica", None)]
    half = [P(None, "model"), P("model", None)] + [P(None, "model")] * 3 + [P("model", None), P(), P()]
    return jax.shard_map(
        local,
        mesh=mesh,
        in_specs=(*slope, *cut, *cut),
        out_specs=(*half, *cut, *cut),
        check_vma=False,
    )
```

```python
import jax
import jax.numpy as jnp
from jax import lax
from jax.experimental import pallas as pl
from jax.experimental.pallas import tpu as pltpu
from jax.sharding import PartitionSpec as P


learn_rate = 0.025
hold_rate = 0.7

B = 64
T = 12 * B + 8
COLS = ((0, 4), (4, 1), (5, 1), (6, 1), (7, 4), (11, 1))
CUT = 4 * 3 * B
AT_VALUE = CUT
AT_DOWN = AT_VALUE + 2 * B
AT_MIXED = AT_DOWN + 512
AT_LAST = AT_MIXED + 128
ROWS = AT_LAST + 8
SCALE = 8192.0
SCALE_VEC = 4096.0
ORDER = (0, 2, 1, 3)


def vmem(x):
    return pltpu.with_memory_space_constraint(x, pltpu.VMEM)


def hbm(x):
    return pltpu.with_memory_space_constraint(x, pltpu.HBM)


VM = pl.BlockSpec(memory_space=pltpu.VMEM)
SM = pl.BlockSpec(memory_space=pltpu.SMEM)
HB = pl.BlockSpec(memory_space=pltpu.HBM)
PARAMS = pltpu.CompilerParams(vmem_limit_bytes=24 << 20)


def send(x, stage, d):
    pairs = []
    for z in range(4):
        for y in range(4):
            for m in range(8):
                along_y = (m % 2 == 0) == (stage == 0)
                to = (z * 4 + (y + d) % 4) if along_y else ((z + d) % 4 * 4 + y)
                pairs.append(((z * 4 + y) * 8 + m, to * 8 + m))
    return lax.ppermute(x, ("replica", "model"), pairs)


def marked(x, d, stage=1):
    return send(x, stage, d)


def block_of(at_ref, f, s):
    c = at_ref[2]
    return f * (1 + 3 * c) + s * (4 - 3 * c)


def pack(place, slopes, distances):
    n = len(distances)

    def kernel(at_ref, up, query, key, value, down, mixed, norm, bias, out_a, out_b, down_s, mixed_s, norm_s, bias_s, sems):
        fi, c = at_ref[0], at_ref[2]
        used = [0]

        def copy(source, target):
            one = pltpu.make_async_copy(source, target, sems.at[used[0]])
            used[0] += 1
            one.start()
            return one

        first = [copy(down.at[0, pl.ds(k * 128, 128)], down_s.at[pl.ds(k * 128, 128)]) for k in range(4)]
        first += [copy(mixed.at[0], mixed_s), copy(norm, norm_s), copy(bias, bias_s)]
        rest = []
        for o, d in enumerate(distances):
            f = (fi + d) & 3
            for s in range(4):
                rows = pl.ds(pl.multiple_of(block_of(at_ref, f, s) * B, B), B)
                target = out_b.at[o, pl.ds(s // 2 * B, B), pl.ds(s % 2 * 128, 128)]
                rest.append(copy(value.at[rows], target))
            ends = [
                (up, slice(0, 256), slice(0, B), slice(0, 256)),
                (up, slice(256, 512), slice(B, 2 * B), slice(0, 256)),
                (query, slice(0, 128), slice(2 * B, 3 * B), slice(0, 128)),
                (key, slice(0, 128), slice(2 * B, 3 * B), slice(128, 256)),
            ]
            for ref, lanes, rows, to in ends:
                at = used[0]
                used[0] += 1

                def one(source, ref=ref, lanes=lanes, rows=rows, to=to, at=at, o=o):
                    return pltpu.make_async_copy(source, out_a.at[o, :, rows, to], sems.at[at])

                @pl.when(c == 0)
                def _(ref=ref, lanes=lanes, one=one, f=f):
                    one(ref.at[:, f, :, lanes]).start()

                @pl.when(c != 0)
                def _(ref=ref, lanes=lanes, one=one, f=f):
                    one(ref.at[f, :, :, lanes]).start()

                rest.append(one(ref.at[0, :, :, lanes]))
        lane = lax.broadcasted_iota(jnp.int32, (B, 128), 1)
        row = lax.broadcasted_iota(jnp.int32, (8, 128), 0)

        def spread(ref, rows, to_row, make):
            for o, d in enumerate(distances):
                f = (fi + d) & 3
                turn_l = jnp.where(c == 0, (f & 1) * 64, 0)
                turn_r = jnp.where(c == 0, 64 - (f & 1) * 64, 0)
                for h in range(2):
                    t_l = jnp.where(c == 0, h * 4 + (f >> 1), f * 2 + h)
                    t_r = jnp.where(c == 0, h * 4 + 2 + (f >> 1), f * 2 + h)
                    left = make(ref, pl.ds(pl.multiple_of(t_l * 128, 128), 128))
                    right = make(ref, pl.ds(pl.multiple_of(t_r * 128, 128), 128))
                    left, right = pltpu.roll(left, turn_l, 1), pltpu.roll(right, turn_r, 1)
                    out_b[o, to_row : to_row + rows, h * 128 : h * 128 + 128] = jnp.where(lane[:rows] < 64, left, right)

        for k in range(10):
            if k < 8 and k % 2 == 0:
                first[k // 2].wait()
            if k == 8:
                for one in first[4:]:
                    one.wait()
            ref, at = (down_s, k * B) if k < 8 else (mixed_s, (k - 8) * B)
            spread(ref, B, AT_DOWN - CUT + k * B, lambda ref, lanes: ref[at : at + B, lanes])

        def last(refs, at):
            n = jnp.broadcast_to(refs[0][0:1, at] * 0.5, (8, 128))
            b = jnp.broadcast_to(refs[1][0:1, at] * 0.5, (8, 128))
            return jnp.where(row == 0, n, jnp.where(row == 1, b, 0.0))

        spread((norm_s, bias_s), 8, AT_LAST - CUT, last)
        for one in rest:
            one.wait()

    f32 = jnp.float32
    up, query, key, value, *others = slopes
    blocks = [x.reshape(4, 4, B, -1) for x in (up, query, key)]
    return pl.pallas_call(
        kernel,
        in_specs=[SM] + [HB] * 8,
        out_specs=(VM, VM),
        out_shape=(pltpu.VMEM((n, 4, 3 * B, 256), f32), pltpu.VMEM((n, ROWS - CUT, 256), f32)),
        scratch_shapes=[
            pltpu.VMEM((512, 1024), f32),
            pltpu.VMEM((128, 1024), f32),
            pltpu.VMEM((1, 1024), f32),
            pltpu.VMEM((1, 1024), f32),
            pltpu.SemaphoreType.DMA((7 + 8 * n,)),
        ],
        compiler_params=PARAMS,
    )(place, *[hbm(x) for x in (*blocks, value[0], *others)])


def turn_kernel(at_ref, a, b, out):
    for s in range(4):
        e = pl.ds((s - at_ref[1]) & 3, 1)
        for k in range(6):
            at = s * 192 + k // 2 * B
            out[e, k * B : k * B + B, :] = a[at : at + B, k % 2 * 128 : k % 2 * 128 + 128][None]
        at = s // 2 * B
        out[e, 6 * B : 7 * B, :] = b[at : at + B, s % 2 * 128 : s % 2 * 128 + 128][None]
    at = AT_DOWN - CUT
    for h in range(2):
        lanes = slice(h * 128, h * 128 + 128)
        tiles = [b[at + k * 128 : at + k * 128 + 128, lanes].T for k in range(5)]
        last = b[AT_LAST - CUT :, lanes]
        for j in range(2):
            e = (2 * h + j - at_ref[1]) & 3
            for k, tile in enumerate(tiles):
                out[pl.ds(e, 1), (7 + k) * B : (8 + k) * B, :] = tile[None, j * B : j * B + B]
            out[pl.ds(e, 1), 12 * B :, :] = (last if j == 0 else pltpu.roll(last, 64, 1))[None]


def turn(place, a, b):
    return pl.pallas_call(
        turn_kernel,
        in_specs=[SM, VM, VM],
        out_specs=VM,
        out_shape=pltpu.VMEM((4, T, 128), jnp.float32),
        compiler_params=PARAMS,
        name="turn",
    )(place, vmem(a), vmem(b))


def norms_kernel(total, p_up, p_query, p_key, p_value, p_down, p_mixed, part):
    lane = lax.broadcasted_iota(jnp.int32, (B, 128), 1)
    params = (p_up, p_query, p_key, p_value, p_down, p_mixed)
    table = jnp.zeros((B, 128), jnp.float32)
    for m, (col, n) in enumerate(COLS):
        squares = jnp.zeros((B, 128), jnp.float32)
        own = jnp.zeros((B, 128), jnp.float32)
        for k in range(n):
            x = total[(col + k) * B : (col + k + 1) * B, :] * (1.0 / SCALE)
            squares = squares + x * x
            p = params[m][:, k * 128 : k * 128 + 128]
            own = own + p * p
        s = jnp.sum(squares, axis=1, keepdims=True)
        o = jnp.sum(own, axis=1, keepdims=True)
        table = jnp.where(lane == m, o, jnp.where(lane == 8 + m, s, table))
    table = jnp.concatenate([table, jnp.zeros((128 - B, 128), jnp.float32)], axis=0)
    table = table.T[:16, :]
    part[...] = table


def norms(total, *params):
    return pl.pallas_call(
        norms_kernel,
        in_specs=[VM] * 7,
        out_specs=VM,
        out_shape=pltpu.VMEM((16, 128), jnp.float32),
        compiler_params=PARAMS,
        name="norms",
    )(vmem(total), *params)


def steps(parts, total, params, states, store, store_half):
    sums = parts[...]
    ratio = jnp.sqrt(sums[:8]) * lax.rsqrt(sums[8:16] + 1e-06)
    ratio = jnp.concatenate([ratio, jnp.zeros((120, 128), jnp.float32)], axis=0).T[:B, :]

    def step(m, param, state):
        new = hold_rate * state + (1.0 - hold_rate) * m * m
        return param - learn_rate * m * lax.rsqrt(new + 1e-06), new

    for i, (col, n) in enumerate(COLS):
        r = ratio[:, i : i + 1]
        for k in range(n):
            at = (col + k) * B
            lanes = slice(k * 128, k * 128 + 128)
            m = total[at : at + B, :] * (1.0 / SCALE) * r
            nxt, new = step(m, params[i][:, lanes], states[i][:, lanes])
            store(i, lanes, nxt, new)
            store_half(at, nxt)
    both = []
    for j in range(2):
        m = total[12 * B + j : 12 * B + j + 1, :B] * (1.0 / SCALE_VEC)
        nxt, new = step(m, params[6 + j][...], states[6 + j][...])
        store(6 + j, slice(None), nxt, new)
        both.append(jnp.concatenate([nxt, nxt], axis=1))
    row = lax.broadcasted_iota(jnp.int32, (8, 128), 0)
    n = jnp.broadcast_to(both[0], (8, 128))
    b = jnp.broadcast_to(both[1], (8, 128))
    store_half(12 * B, jnp.where(row == 0, n, jnp.where(row == 1, b, 0.0)))


def halves_kernel(parts, total, *refs):
    half = refs[16]

    def store_half(at, nxt):
        half[at : at + nxt.shape[0], :] = nxt.astype(jnp.bfloat16)

    steps(parts, total, refs[:8], refs[8:16], lambda *_: None, store_half)


def halves(parts, total, params, states):
    return pl.pallas_call(
        halves_kernel,
        in_specs=[VM] * 18,
        out_specs=VM,
        out_shape=pltpu.VMEM((T, 128), jnp.bfloat16),
        compiler_params=PARAMS,
        name="halves",
    )(vmem(parts), vmem(total), *params, *states)


def update_kernel(parts, total, *refs):
    nexts, news = refs[16:24], refs[24:32]

    def store(i, lanes, nxt, new):
        nexts[i][:, lanes] = nxt
        news[i][:, lanes] = new

    steps(parts, total, refs[:8], refs[8:16], store, lambda *_: None)


def update(parts, total, params, states):
    shapes = [jax.ShapeDtypeStruct(p.shape, jnp.float32) for p in params]
    out = pl.pallas_call(
        update_kernel,
        in_specs=[VM] * 18,
        out_shape=(*shapes, *shapes),
        compiler_params=PARAMS,
        name="update",
    )(vmem(parts), vmem(total), *params, *states)
    return out[:8], out[8:]


def early_kernel(at_ref, *refs):
    stacks = {0: refs[0:2], 1: refs[2:4], 3: refs[4:6]}
    up, query, key, value, down_s, mixed_s, vectors, up_s, query_s, key_s, value_s, rest_s, sems = refs[6:]
    for d in range(4):
        for k, e in enumerate(ORDER):
            r = block_of(at_ref, (at_ref[0] - d) & 3, (at_ref[1] - e) & 3)
            rows = pl.ds(pl.multiple_of(r * B, B), B)
            block = stacks[d][k // 2][k % 2] if d != 2 else jnp.zeros((T, 128), jnp.bfloat16)
            for c in range(4):
                up_s[rows, c * 128 : c * 128 + 128] = block[c * B : c * B + B, :]
            query_s[rows, :] = block[4 * B : 5 * B, :]
            key_s[rows, :] = block[5 * B : 6 * B, :]
            value_s[rows, :] = block[6 * B : 7 * B, :]
            rest_s[pl.ds(r, 1)] = block[7 * B :, :][None]
    pairs = ((up_s, up), (query_s, query), (key_s, key), (value_s, value))
    copies = [pltpu.make_async_copy(x, y, sems.at[k]) for k, (x, y) in enumerate(pairs)]
    for one in copies:
        one.start()
    lane = lax.broadcasted_iota(jnp.int32, (8, 128), 1)
    for p in range(8):
        lanes = slice(p * 128, p * 128 + 128)
        for k in range(5):
            tile = jnp.concatenate([rest_s[2 * p + j, k * B : k * B + B, :] for j in range(2)], axis=0).T
            if k < 4:
                down_s[k * 128 : k * 128 + 128, lanes] = tile
            else:
                mixed_s[:, lanes] = tile
        both = [rest_s[2 * p + j, 5 * B :, :].astype(jnp.float32) for j in range(2)]
        last = jnp.where(lane < B, both[0], both[1])
        vectors[p : p + 1, :] = last[0:1]
        vectors[8 + p : 9 + p, :] = last[1:2]
    for one in copies:
        one.wait()


def late_kernel(at_ref, a, b, *refs):
    up, query, key, value, down_s, mixed_s, vectors, down, mixed, up_s, thin_s, sems = refs[7:]
    copies = []

    def copy(source, target):
        copies.append(pltpu.make_async_copy(source, target, sems.at[len(copies)]))
        copies[-1].start()

    half = lax.broadcasted_iota(jnp.int32, (128, 128), 1) >> 6
    for i, e in enumerate(ORDER):
        block = (a, b)[i // 2].at[i % 2]
        r = block_of(at_ref, (at_ref[0] - 2) & 3, (at_ref[1] - e) & 3)
        rows = pl.ds(pl.multiple_of(r * B, B), B)
        for c in range(4):
            up_s[i, :, c * 128 : c * 128 + 128] = block[c * B : c * B + B, :]
        copy(up_s.at[i], up.at[rows])
        for c, target in enumerate((query, key, value)):
            thin_s[i, c] = block[(4 + c) * B : (5 + c) * B, :]
            copy(thin_s.at[i, c], target.at[rows])
        lanes = pl.ds(pl.multiple_of((r >> 1) * 128, 128), 128)
        mine = half == (r & 1)
        for k in range(5):
            one = block[(7 + k) * B : (8 + k) * B, :]
            tile = jnp.concatenate([one, one], axis=0).T.astype(jnp.float32)
            ref, to = (down_s, slice(k * 128, k * 128 + 128)) if k < 4 else (mixed_s, slice(None))
            ref[to, lanes] = jnp.where(mine, tile, ref[to, lanes].astype(jnp.float32)).astype(jnp.bfloat16)
        last = block[12 * B :, :].astype(jnp.float32)
        for k in range(2):
            to = pl.ds(k * 8 + (r >> 1), 1)
            vectors[to, :] = jnp.where(mine[0:1], last[k : k + 1], vectors[to, :])
    copy(down_s, down)
    copy(mixed_s, mixed)
    for one in copies:
        one.wait()


def unpack(place, early, late):
    bf16 = jnp.bfloat16
    shapes = ((1024, 512), (1024, 128), (1024, 128), (1024, 128), (512, 1024), (128, 1024))
    outs = [jax.ShapeDtypeStruct(s, bf16) for s in shapes]
    kept = [pltpu.VMEM(s, bf16) for s in shapes[4:]] + [pltpu.VMEM((16, 128), jnp.float32)]
    first = pl.pallas_call(
        early_kernel,
        in_specs=[SM] + [VM] * 6,
        out_specs=(*[HB] * 4, *[VM] * 3),
        out_shape=(*outs[:4], *kept),
        scratch_shapes=[
            *[pltpu.VMEM(s, bf16) for s in shapes[:4]],
            pltpu.VMEM((16, 5 * B + 8, 128), bf16),
            pltpu.SemaphoreType.DMA((4,)),
        ],
        compiler_params=PARAMS,
        name="unpack_early",
    )(place, *[vmem(x) for x in early])
    up, query, key, value, _, _, vectors, down, mixed = pl.pallas_call(
        late_kernel,
        in_specs=[SM, VM, VM] + [HB] * 4 + [VM] * 3,
        out_specs=(*[HB] * 4, *[VM] * 3, HB, HB),
        out_shape=(*outs[:4], *kept, *outs[4:]),
        input_output_aliases={3 + k: k for k in range(7)},
        scratch_shapes=[
            pltpu.VMEM((4, B, 512), bf16),
            pltpu.VMEM((4, 3, B, 128), bf16),
            pltpu.SemaphoreType.DMA((18,)),
        ],
        compiler_params=PARAMS,
        name="unpack_late",
    )(place, *[vmem(x) for x in late], *[hbm(x) for x in first[:4]], *[vmem(x) for x in first[4:]])
    return up, query, key, value, down, mixed, vectors


def local(*args):
    f16, f32, bf16 = jnp.float16, jnp.float32, jnp.bfloat16
    at = lax.axis_index("replica").astype(jnp.int32)
    core = lax.axis_index("model").astype(jnp.int32) & 1
    zi, yi = at >> 2, at & 3
    place = jnp.stack([jnp.where(core == 0, yi, zi), jnp.where(core == 0, zi, yi), core])

    def inner(xs):
        up, down, query, key, value, mixed, norm, bias = xs
        return up, query, key, value, down, mixed, norm, bias

    def turned(xs):
        up, query, key, value, down, mixed, norm, bias = inner(xs)
        return [vmem(x) for x in (up, query, key, value, down.T, mixed.T, norm[None], bias[None])]

    slopes, params, states = inner(args[:8]), turned(args[8:16]), turned(args[16:24])

    packed_a, packed_b = pack(place, slopes, ORDER[1:])
    two_a, one_a, three_a = [packed_a[o].reshape(CUT, 256) * SCALE for o in range(3)]
    two_b, one_b, three_b = [packed_b[o] * SCALE for o in range(3)]
    out = [x.astype(f16) for x in (two_a, two_b, one_b, three_a)]
    got = [send(x, 0, d) for x, d in zip(out, (1, 3, 1, 3))]
    mid_a = ((one_a + got[0].astype(f32)) * 0.5).astype(f16)
    mid_b = ((three_b + got[1].astype(f32)) * 0.5).astype(f16)
    through = send(mid_a, 0, 1), send(mid_b, 0, 3)
    later = lax.optimization_barrier((place, mid_a, mid_b))[0]
    own_a, own_b = pack(later, slopes, (0,))
    four_a = (own_a.reshape(CUT, 256) * SCALE + got[3].astype(f32) + 2.0 * through[0].astype(f32)) * 0.25
    four_b = (own_b[0] * SCALE + got[2].astype(f32) + 2.0 * through[1].astype(f32)) * 0.25
    four = turn(place, four_a, four_b)
    total = four[0] + sum(marked(four[e].astype(f16), e).astype(f32) for e in ORDER[1:])

    parts = norms(total, *params[:6])
    for partner in (lambda m: m ^ 1, lambda m: m ^ 2, lambda m: m ^ 6):
        parts = parts + lax.ppermute(parts, "model", [(m, partner(m)) for m in range(8)])
    half = halves(parts, total, params, states)

    row = [half] + [marked(half, e) for e in ORDER[1:]]
    own_a, own_b = jnp.stack(row[:2]), jnp.stack(row[2:])
    one_a, three_a = marked(own_a, 1, 0), marked(own_a, 3, 0)
    three_b, one_b = marked(own_b, 3, 0), marked(own_b, 1, 0)
    two_a, two_b = send(one_a, 0, 1), send(three_b, 0, 3)
    nexts, news = update(lax.optimization_barrier((parts, own_a, own_b))[0], total, params, states)
    up, query, key, value, down, mixed, vectors = unpack(place, (own_a, own_b, one_a, one_b, three_a, three_b), (two_a, two_b))
    vectors = vectors.astype(bf16)
    norm, bias = vectors[:8].reshape(1024), vectors[8:].reshape(1024)

    def outer(xs):
        up, query, key, value, down, mixed, norm, bias = xs
        return up, down.T, query, key, value, mixed.T, norm[0], bias[0]

    return (up, down, query, key, value, mixed, norm, bias, *outer(nexts), *outer(news))


def solution(mesh):
    cut = [P("replica", "model"), P("model", "replica")] + [P("replica", "model")] * 3
    cut += [P("model", "replica"), P("replica"), P("replica")]
    slope = [P("replica", None, "model"), P("replica", "model", None)] + [P("replica", None, "model")] * 3
    slope += [P("replica", "model", None), P("replica", None), P("replica", None)]
    half = [P(None, "model"), P("model", None)] + [P(None, "model")] * 3 + [P("model", None), P(), P()]
    return jax.shard_map(
        local,
        mesh=mesh,
        in_specs=(*slope, *cut, *cut),
        out_specs=(*half, *cut, *cut),
        check_vma=False,
    )
```

```python
import jax
import jax.numpy as jnp
from jax import lax
from jax.experimental import pallas as pl
from jax.experimental.pallas import tpu as pltpu
from jax.sharding import PartitionSpec as P


learn_rate = 0.025
hold_rate = 0.7

B = 64
T = 12 * B + 8
COLS = ((0, 4), (4, 1), (5, 1), (6, 1), (7, 4), (11, 1))
CUT = 4 * 3 * B
AT_VALUE = CUT
AT_DOWN = AT_VALUE + 2 * B
AT_MIXED = AT_DOWN + 512
AT_LAST = AT_MIXED + 128
ROWS = AT_LAST + 8
SCALE = 8192.0
SCALE_VEC = 4096.0
ORDER = (0, 2, 1, 3)


def vmem(x):
    return pltpu.with_memory_space_constraint(x, pltpu.VMEM)


def hbm(x):
    return pltpu.with_memory_space_constraint(x, pltpu.HBM)


VM = pl.BlockSpec(memory_space=pltpu.VMEM)
SM = pl.BlockSpec(memory_space=pltpu.SMEM)
HB = pl.BlockSpec(memory_space=pltpu.HBM)
PARAMS = pltpu.CompilerParams(vmem_limit_bytes=24 << 20)


def send(x, stage, d):
    pairs = []
    for z in range(4):
        for y in range(4):
            for m in range(8):
                along_y = (m % 2 == 0) == (stage == 0)
                to = (z * 4 + (y + d) % 4) if along_y else ((z + d) % 4 * 4 + y)
                pairs.append(((z * 4 + y) * 8 + m, to * 8 + m))
    return lax.ppermute(x, ("replica", "model"), pairs)


def marked(x, d, stage=1):
    return send(x, stage, d)


def block_of(at_ref, f, s):
    c = at_ref[2]
    return f * (1 + 3 * c) + s * (4 - 3 * c)


def pack(place, slopes, distances):
    n = len(distances)

    def kernel(at_ref, up, query, key, value, down, mixed, norm, bias, out_a, out_b, down_s, mixed_s, norm_s, bias_s, sems):
        fi, c = at_ref[0], at_ref[2]
        used = [0]

        def copy(source, target):
            one = pltpu.make_async_copy(source, target, sems.at[used[0]])
            used[0] += 1
            one.start()
            return one

        first = [copy(down.at[0, pl.ds(k * 128, 128)], down_s.at[pl.ds(k * 128, 128)]) for k in range(4)]
        first += [copy(mixed.at[0], mixed_s), copy(norm, norm_s), copy(bias, bias_s)]
        rest = []
        for o, d in enumerate(distances):
            f = (fi + d) & 3
            for s in range(4):
                rows = pl.ds(pl.multiple_of(block_of(at_ref, f, s) * B, B), B)
                target = out_b.at[o, pl.ds(s // 2 * B, B), pl.ds(s % 2 * 128, 128)]
                rest.append(copy(value.at[rows], target))
            ends = [
                (up, slice(0, 256), slice(0, B), slice(0, 256)),
                (up, slice(256, 512), slice(B, 2 * B), slice(0, 256)),
                (query, slice(0, 128), slice(2 * B, 3 * B), slice(0, 128)),
                (key, slice(0, 128), slice(2 * B, 3 * B), slice(128, 256)),
            ]
            for ref, lanes, rows, to in ends:
                at = used[0]
                used[0] += 1

                def one(source, ref=ref, lanes=lanes, rows=rows, to=to, at=at, o=o):
                    return pltpu.make_async_copy(source, out_a.at[o, :, rows, to], sems.at[at])

                @pl.when(c == 0)
                def _(ref=ref, lanes=lanes, one=one, f=f):
                    one(ref.at[:, f, :, lanes]).start()

                @pl.when(c != 0)
                def _(ref=ref, lanes=lanes, one=one, f=f):
                    one(ref.at[f, :, :, lanes]).start()

                rest.append(one(ref.at[0, :, :, lanes]))
        lane = lax.broadcasted_iota(jnp.int32, (B, 128), 1)
        row = lax.broadcasted_iota(jnp.int32, (8, 128), 0)

        def spread(ref, rows, to_row, make):
            for o, d in enumerate(distances):
                f = (fi + d) & 3
                turn_l = jnp.where(c == 0, (f & 1) * 64, 0)
                turn_r = jnp.where(c == 0, 64 - (f & 1) * 64, 0)
                for h in range(2):
                    t_l = jnp.where(c == 0, h * 4 + (f >> 1), f * 2 + h)
                    t_r = jnp.where(c == 0, h * 4 + 2 + (f >> 1), f * 2 + h)
                    left = make(ref, pl.ds(pl.multiple_of(t_l * 128, 128), 128))
                    right = make(ref, pl.ds(pl.multiple_of(t_r * 128, 128), 128))
                    left, right = pltpu.roll(left, turn_l, 1), pltpu.roll(right, turn_r, 1)
                    out_b[o, to_row : to_row + rows, h * 128 : h * 128 + 128] = jnp.where(lane[:rows] < 64, left, right)

        for k in range(10):
            if k < 8 and k % 2 == 0:
                first[k // 2].wait()
            if k == 8:
                for one in first[4:]:
                    one.wait()
            ref, at = (down_s, k * B) if k < 8 else (mixed_s, (k - 8) * B)
            spread(ref, B, AT_DOWN - CUT + k * B, lambda ref, lanes: ref[at : at + B, lanes])

        def last(refs, at):
            n = jnp.broadcast_to(refs[0][0:1, at] * 0.5, (8, 128))
            b = jnp.broadcast_to(refs[1][0:1, at] * 0.5, (8, 128))
            return jnp.where(row == 0, n, jnp.where(row == 1, b, 0.0))

        spread((norm_s, bias_s), 8, AT_LAST - CUT, last)
        for one in rest:
            one.wait()

    f32 = jnp.float32
    up, query, key, value, *others = slopes
    blocks = [x.reshape(4, 4, B, -1) for x in (up, query, key)]
    return pl.pallas_call(
        kernel,
        in_specs=[SM] + [HB] * 8,
        out_specs=(VM, VM),
        out_shape=(pltpu.VMEM((n, 4, 3 * B, 256), f32), pltpu.VMEM((n, ROWS - CUT, 256), f32)),
        scratch_shapes=[
            pltpu.VMEM((512, 1024), f32),
            pltpu.VMEM((128, 1024), f32),
            pltpu.VMEM((1, 1024), f32),
            pltpu.VMEM((1, 1024), f32),
            pltpu.SemaphoreType.DMA((7 + 8 * n,)),
        ],
        compiler_params=PARAMS,
    )(place, *[hbm(x) for x in (*blocks, value[0], *others)])


def turn_kernel(at_ref, a, b, out):
    for s in range(4):
        e = pl.ds((s - at_ref[1]) & 3, 1)
        for k in range(6):
            at = s * 192 + k // 2 * B
            out[e, k * B : k * B + B, :] = a[at : at + B, k % 2 * 128 : k % 2 * 128 + 128][None]
        at = s // 2 * B
        out[e, 6 * B : 7 * B, :] = b[at : at + B, s % 2 * 128 : s % 2 * 128 + 128][None]
    at = AT_DOWN - CUT
    for h in range(2):
        lanes = slice(h * 128, h * 128 + 128)
        tiles = [b[at + k * 128 : at + k * 128 + 128, lanes].T for k in range(5)]
        last = b[AT_LAST - CUT :, lanes]
        for j in range(2):
            e = (2 * h + j - at_ref[1]) & 3
            for k, tile in enumerate(tiles):
                out[pl.ds(e, 1), (7 + k) * B : (8 + k) * B, :] = tile[None, j * B : j * B + B]
            out[pl.ds(e, 1), 12 * B :, :] = (last if j == 0 else pltpu.roll(last, 64, 1))[None]


def turn(place, a, b):
    return pl.pallas_call(
        turn_kernel,
        in_specs=[SM, VM, VM],
        out_specs=VM,
        out_shape=pltpu.VMEM((4, T, 128), jnp.float32),
        compiler_params=PARAMS,
        name="turn",
    )(place, vmem(a), vmem(b))


def norms_kernel(total, p_up, p_query, p_key, p_value, p_down, p_mixed, part):
    lane = lax.broadcasted_iota(jnp.int32, (B, 128), 1)
    params = (p_up, p_query, p_key, p_value, p_down, p_mixed)
    table = jnp.zeros((B, 128), jnp.float32)
    for m, (col, n) in enumerate(COLS):
        squares = jnp.zeros((B, 128), jnp.float32)
        own = jnp.zeros((B, 128), jnp.float32)
        for k in range(n):
            x = total[(col + k) * B : (col + k + 1) * B, :] * (1.0 / SCALE)
            squares = squares + x * x
            p = params[m][:, k * 128 : k * 128 + 128]
            own = own + p * p
        s = jnp.sum(squares, axis=1, keepdims=True)
        o = jnp.sum(own, axis=1, keepdims=True)
        table = jnp.where(lane == m, o, jnp.where(lane == 8 + m, s, table))
    table = jnp.concatenate([table, jnp.zeros((128 - B, 128), jnp.float32)], axis=0)
    table = table.T[:16, :]
    for r in range(part.shape[0]):
        part[r] = table


def norms(copies, total, *params):
    return pl.pallas_call(
        norms_kernel,
        in_specs=[VM] * 7,
        out_specs=VM,
        out_shape=pltpu.VMEM((copies, 16, 128), jnp.float32),
        compiler_params=PARAMS,
        name="norms",
    )(vmem(total), *params)


def steps(parts, total, params, states, store, store_half):
    sums = parts[0]
    for d in range(1, parts.shape[0]):
        sums = sums + parts[d]
    ratio = jnp.sqrt(sums[:8]) * lax.rsqrt(sums[8:16] + 1e-06)
    ratio = jnp.concatenate([ratio, jnp.zeros((120, 128), jnp.float32)], axis=0).T[:B, :]

    def step(m, param, state):
        new = hold_rate * state + (1.0 - hold_rate) * m * m
        return param - learn_rate * m * lax.rsqrt(new + 1e-06), new

    for i, (col, n) in enumerate(COLS):
        r = ratio[:, i : i + 1]
        for k in range(n):
            at = (col + k) * B
            lanes = slice(k * 128, k * 128 + 128)
            m = total[at : at + B, :] * (1.0 / SCALE) * r
            nxt, new = step(m, params[i][:, lanes], states[i][:, lanes])
            store(i, lanes, nxt, new)
            store_half(at, nxt)
    both = []
    for j in range(2):
        m = total[12 * B + j : 12 * B + j + 1, :B] * (1.0 / SCALE_VEC)
        nxt, new = step(m, params[6 + j][...], states[6 + j][...])
        store(6 + j, slice(None), nxt, new)
        both.append(jnp.concatenate([nxt, nxt], axis=1))
    row = lax.broadcasted_iota(jnp.int32, (8, 128), 0)
    n = jnp.broadcast_to(both[0], (8, 128))
    b = jnp.broadcast_to(both[1], (8, 128))
    store_half(12 * B, jnp.where(row == 0, n, jnp.where(row == 1, b, 0.0)))


def halves_kernel(parts, total, *refs):
    half = refs[16]

    def store_half(at, nxt):
        half[at : at + nxt.shape[0], :] = nxt.astype(jnp.bfloat16)

    steps(parts, total, refs[:8], refs[8:16], lambda *_: None, store_half)


def halves(parts, total, params, states):
    return pl.pallas_call(
        halves_kernel,
        in_specs=[VM] * 18,
        out_specs=VM,
        out_shape=pltpu.VMEM((T, 128), jnp.bfloat16),
        compiler_params=PARAMS,
        name="halves",
    )(vmem(parts), vmem(total), *params, *states)


def update_kernel(parts, total, *refs):
    nexts, news = refs[16:24], refs[24:32]

    def store(i, lanes, nxt, new):
        nexts[i][:, lanes] = nxt
        news[i][:, lanes] = new

    steps(parts, total, refs[:8], refs[8:16], store, lambda *_: None)


def update(parts, total, params, states):
    shapes = [jax.ShapeDtypeStruct(p.shape, jnp.float32) for p in params]
    out = pl.pallas_call(
        update_kernel,
        in_specs=[VM] * 18,
        out_shape=(*shapes, *shapes),
        compiler_params=PARAMS,
        name="update",
    )(vmem(parts), vmem(total), *params, *states)
    return out[:8], out[8:]


def early_kernel(at_ref, *refs):
    stacks = {0: refs[0:2], 1: refs[2:4], 3: refs[4:6]}
    up, query, key, value, down_s, mixed_s, vectors, up_s, query_s, key_s, value_s, rest_s, sems = refs[6:]
    for d in range(4):
        for k, e in enumerate(ORDER):
            r = block_of(at_ref, (at_ref[0] - d) & 3, (at_ref[1] - e) & 3)
            rows = pl.ds(pl.multiple_of(r * B, B), B)
            block = stacks[d][k // 2][k % 2] if d != 2 else jnp.zeros((T, 128), jnp.bfloat16)
            for c in range(4):
                up_s[rows, c * 128 : c * 128 + 128] = block[c * B : c * B + B, :]
            query_s[rows, :] = block[4 * B : 5 * B, :]
            key_s[rows, :] = block[5 * B : 6 * B, :]
            value_s[rows, :] = block[6 * B : 7 * B, :]
            rest_s[pl.ds(r, 1)] = block[7 * B :, :][None]
    pairs = ((up_s, up), (query_s, query), (key_s, key), (value_s, value))
    copies = [pltpu.make_async_copy(x, y, sems.at[k]) for k, (x, y) in enumerate(pairs)]
    for one in copies:
        one.start()
    lane = lax.broadcasted_iota(jnp.int32, (8, 128), 1)
    for p in range(8):
        lanes = slice(p * 128, p * 128 + 128)
        for k in range(5):
            tile = jnp.concatenate([rest_s[2 * p + j, k * B : k * B + B, :] for j in range(2)], axis=0).T
            if k < 4:
                down_s[k * 128 : k * 128 + 128, lanes] = tile
            else:
                mixed_s[:, lanes] = tile
        both = [rest_s[2 * p + j, 5 * B :, :].astype(jnp.float32) for j in range(2)]
        last = jnp.where(lane < B, both[0], both[1])
        vectors[p : p + 1, :] = last[0:1]
        vectors[8 + p : 9 + p, :] = last[1:2]
    for one in copies:
        one.wait()


def late_kernel(at_ref, a, b, *refs):
    up, query, key, value, down_s, mixed_s, vectors, down, mixed, up_s, thin_s, sems = refs[7:]
    copies = []

    def copy(source, target):
        copies.append(pltpu.make_async_copy(source, target, sems.at[len(copies)]))
        copies[-1].start()

    half = lax.broadcasted_iota(jnp.int32, (128, 128), 1) >> 6
    for i, e in enumerate(ORDER):
        block = (a, b)[i // 2].at[i % 2]
        r = block_of(at_ref, (at_ref[0] - 2) & 3, (at_ref[1] - e) & 3)
        rows = pl.ds(pl.multiple_of(r * B, B), B)
        for c in range(4):
            up_s[i, :, c * 128 : c * 128 + 128] = block[c * B : c * B + B, :]
        copy(up_s.at[i], up.at[rows])
        for c, target in enumerate((query, key, value)):
            thin_s[i, c] = block[(4 + c) * B : (5 + c) * B, :]
            copy(thin_s.at[i, c], target.at[rows])
        lanes = pl.ds(pl.multiple_of((r >> 1) * 128, 128), 128)
        mine = half == (r & 1)
        for k in range(5):
            one = block[(7 + k) * B : (8 + k) * B, :]
            tile = jnp.concatenate([one, one], axis=0).T.astype(jnp.float32)
            ref, to = (down_s, slice(k * 128, k * 128 + 128)) if k < 4 else (mixed_s, slice(None))
            ref[to, lanes] = jnp.where(mine, tile, ref[to, lanes].astype(jnp.float32)).astype(jnp.bfloat16)
        last = block[12 * B :, :].astype(jnp.float32)
        for k in range(2):
            to = pl.ds(k * 8 + (r >> 1), 1)
            vectors[to, :] = jnp.where(mine[0:1], last[k : k + 1], vectors[to, :])
    copy(down_s, down)
    copy(mixed_s, mixed)
    for one in copies:
        one.wait()


def unpack(place, early, late):
    bf16 = jnp.bfloat16
    shapes = ((1024, 512), (1024, 128), (1024, 128), (1024, 128), (512, 1024), (128, 1024))
    outs = [jax.ShapeDtypeStruct(s, bf16) for s in shapes]
    kept = [pltpu.VMEM(s, bf16) for s in shapes[4:]] + [pltpu.VMEM((16, 128), jnp.float32)]
    first = pl.pallas_call(
        early_kernel,
        in_specs=[SM] + [VM] * 6,
        out_specs=(*[HB] * 4, *[VM] * 3),
        out_shape=(*outs[:4], *kept),
        scratch_shapes=[
            *[pltpu.VMEM(s, bf16) for s in shapes[:4]],
            pltpu.VMEM((16, 5 * B + 8, 128), bf16),
            pltpu.SemaphoreType.DMA((4,)),
        ],
        compiler_params=PARAMS,
        name="unpack_early",
    )(place, *[vmem(x) for x in early])
    up, query, key, value, _, _, vectors, down, mixed = pl.pallas_call(
        late_kernel,
        in_specs=[SM, VM, VM] + [HB] * 4 + [VM] * 3,
        out_specs=(*[HB] * 4, *[VM] * 3, HB, HB),
        out_shape=(*outs[:4], *kept, *outs[4:]),
        input_output_aliases={3 + k: k for k in range(7)},
        scratch_shapes=[
            pltpu.VMEM((4, B, 512), bf16),
            pltpu.VMEM((4, 3, B, 128), bf16),
            pltpu.SemaphoreType.DMA((18,)),
        ],
        compiler_params=PARAMS,
        name="unpack_late",
    )(place, *[vmem(x) for x in late], *[hbm(x) for x in first[:4]], *[vmem(x) for x in first[4:]])
    return up, query, key, value, down, mixed, vectors


def local(*args):
    f16, f32, bf16 = jnp.float16, jnp.float32, jnp.bfloat16
    at = lax.axis_index("replica").astype(jnp.int32)
    core = lax.axis_index("model").astype(jnp.int32) & 1
    zi, yi = at >> 2, at & 3
    place = jnp.stack([jnp.where(core == 0, yi, zi), jnp.where(core == 0, zi, yi), core])

    def inner(xs):
        up, down, query, key, value, mixed, norm, bias = xs
        return up, query, key, value, down, mixed, norm, bias

    def turned(xs):
        up, query, key, value, down, mixed, norm, bias = inner(xs)
        return [vmem(x) for x in (up, query, key, value, down.T, mixed.T, norm[None], bias[None])]

    slopes, params, states = inner(args[:8]), turned(args[8:16]), turned(args[16:24])

    packed_a, packed_b = pack(place, slopes, ORDER[1:])
    two_a, one_a, three_a = [packed_a[o].reshape(CUT, 256) * SCALE for o in range(3)]
    two_b, one_b, three_b = [packed_b[o] * SCALE for o in range(3)]
    out = [x.astype(f16) for x in (two_a, two_b, one_b, three_a)]
    got = [send(x, 0, d) for x, d in zip(out, (1, 3, 1, 3))]
    mid_a = ((one_a + got[0].astype(f32)) * 0.5).astype(f16)
    mid_b = ((three_b + got[1].astype(f32)) * 0.5).astype(f16)
    through = send(mid_a, 0, 1), send(mid_b, 0, 3)
    later = lax.optimization_barrier((place, mid_a, mid_b))[0]
    own_a, own_b = pack(later, slopes, (0,))
    four_a = (own_a.reshape(CUT, 256) * SCALE + got[3].astype(f32) + 2.0 * through[0].astype(f32)) * 0.25
    four_b = (own_b[0] * SCALE + got[2].astype(f32) + 2.0 * through[1].astype(f32)) * 0.25
    four = turn(place, four_a, four_b)
    total = four[0] + sum(marked(four[e].astype(f16), e).astype(f32) for e in ORDER[1:])

    part = norms(lax.axis_size("model"), total, *params[:6])
    parts = lax.all_to_all(part, "model", 0, 0, tiled=True)
    half = halves(parts, total, params, states)

    row = [half] + [marked(half, e) for e in ORDER[1:]]
    own_a, own_b = jnp.stack(row[:2]), jnp.stack(row[2:])
    one_a, three_a = marked(own_a, 1, 0), marked(own_a, 3, 0)
    three_b, one_b = marked(own_b, 3, 0), marked(own_b, 1, 0)
    two_a, two_b = send(one_a, 0, 1), send(three_b, 0, 3)
    nexts, news = update(lax.optimization_barrier((parts, own_a, own_b))[0], total, params, states)
    up, query, key, value, down, mixed, vectors = unpack(place, (own_a, own_b, one_a, one_b, three_a, three_b), (two_a, two_b))
    vectors = vectors.astype(bf16)
    norm, bias = vectors[:8].reshape(1024), vectors[8:].reshape(1024)

    def outer(xs):
        up, query, key, value, down, mixed, norm, bias = xs
        return up, down.T, query, key, value, mixed.T, norm[0], bias[0]

    return (up, down, query, key, value, mixed, norm, bias, *outer(nexts), *outer(news))


def solution(mesh):
    cut = [P("replica", "model"), P("model", "replica")] + [P("replica", "model")] * 3
    cut += [P("model", "replica"), P("replica"), P("replica")]
    slope = [P("replica", None, "model"), P("replica", "model", None)] + [P("replica", None, "model")] * 3
    slope += [P("replica", "model", None), P("replica", None), P("replica", None)]
    half = [P(None, "model"), P("model", None)] + [P(None, "model")] * 3 + [P("model", None), P(), P()]
    return jax.shard_map(
        local,
        mesh=mesh,
        in_specs=(*slope, *cut, *cut),
        out_specs=(*half, *cut, *cut),
        check_vma=False,
    )
```

```python
import jax
import jax.numpy as jnp
from jax import lax
from jax.experimental import pallas as pl
from jax.experimental.pallas import tpu as pltpu
from jax.sharding import PartitionSpec as P


learn_rate = 0.025
hold_rate = 0.7

B = 64
T = 12 * B + 8
COLS = ((0, 4), (4, 1), (5, 1), (6, 1), (7, 4), (11, 1))
CUT = 4 * 3 * B
AT_VALUE = CUT
AT_DOWN = AT_VALUE + 2 * B
AT_MIXED = AT_DOWN + 512
AT_LAST = AT_MIXED + 128
ROWS = AT_LAST + 8
SCALE = 8192.0
SCALE_VEC = 4096.0
ORDER = (0, 2, 1, 3)

GATHER = (0, 2, 3, 1)


def vmem(x):
    return pltpu.with_memory_space_constraint(x, pltpu.VMEM)


def hbm(x):
    return pltpu.with_memory_space_constraint(x, pltpu.HBM)


VM = pl.BlockSpec(memory_space=pltpu.VMEM)
SM = pl.BlockSpec(memory_space=pltpu.SMEM)
HB = pl.BlockSpec(memory_space=pltpu.HBM)
PARAMS = pltpu.CompilerParams(vmem_limit_bytes=24 << 20)


def send(x, stage, d):
    pairs = []
    for z in range(4):
        for y in range(4):
            for m in range(8):
                along_y = (m % 2 == 0) == (stage == 0)
                to = (z * 4 + (y + d) % 4) if along_y else ((z + d) % 4 * 4 + y)
                pairs.append(((z * 4 + y) * 8 + m, to * 8 + m))
    return lax.ppermute(x, ("replica", "model"), pairs)


def marked(x, d, stage=1):
    return send(x, stage, d)


def block_of(at_ref, f, s):
    c = at_ref[2]
    return f * (1 + 3 * c) + s * (4 - 3 * c)


def pack(place, slopes, distances):
    n = len(distances)

    def kernel(at_ref, up, query, key, value, down, mixed, norm, bias, out_a, out_b, down_s, mixed_s, norm_s, bias_s, sems):
        fi, c = at_ref[0], at_ref[2]
        used = [0]

        def copy(source, target):
            one = pltpu.make_async_copy(source, target, sems.at[used[0]])
            used[0] += 1
            one.start()
            return one

        first = [copy(down.at[0, pl.ds(k * 128, 128)], down_s.at[pl.ds(k * 128, 128)]) for k in range(4)]
        first += [copy(mixed.at[0], mixed_s), copy(norm, norm_s), copy(bias, bias_s)]
        rest = []
        for o, d in enumerate(distances):
            f = (fi + d) & 3
            for s in range(4):
                rows = pl.ds(pl.multiple_of(block_of(at_ref, f, s) * B, B), B)
                target = out_b.at[o, pl.ds(s // 2 * B, B), pl.ds(s % 2 * 128, 128)]
                rest.append(copy(value.at[rows], target))
            ends = [
                (up, slice(0, 256), slice(0, B), slice(0, 256)),
                (up, slice(256, 512), slice(B, 2 * B), slice(0, 256)),
                (query, slice(0, 128), slice(2 * B, 3 * B), slice(0, 128)),
                (key, slice(0, 128), slice(2 * B, 3 * B), slice(128, 256)),
            ]
            for ref, lanes, rows, to in ends:
                at = used[0]
                used[0] += 1

                def one(source, ref=ref, lanes=lanes, rows=rows, to=to, at=at, o=o):
                    return pltpu.make_async_copy(source, out_a.at[o, :, rows, to], sems.at[at])

                @pl.when(c == 0)
                def _(ref=ref, lanes=lanes, one=one, f=f):
                    one(ref.at[:, f, :, lanes]).start()

                @pl.when(c != 0)
                def _(ref=ref, lanes=lanes, one=one, f=f):
                    one(ref.at[f, :, :, lanes]).start()

                rest.append(one(ref.at[0, :, :, lanes]))
        lane = lax.broadcasted_iota(jnp.int32, (B, 128), 1)
        row = lax.broadcasted_iota(jnp.int32, (8, 128), 0)

        def spread(ref, rows, to_row, make):
            for o, d in enumerate(distances):
                f = (fi + d) & 3
                turn_l = jnp.where(c == 0, (f & 1) * 64, 0)
                turn_r = jnp.where(c == 0, 64 - (f & 1) * 64, 0)
                for h in range(2):
                    t_l = jnp.where(c == 0, h * 4 + (f >> 1), f * 2 + h)
                    t_r = jnp.where(c == 0, h * 4 + 2 + (f >> 1), f * 2 + h)
                    left = make(ref, pl.ds(pl.multiple_of(t_l * 128, 128), 128))
                    right = make(ref, pl.ds(pl.multiple_of(t_r * 128, 128), 128))
                    left, right = pltpu.roll(left, turn_l, 1), pltpu.roll(right, turn_r, 1)
                    out_b[o, to_row : to_row + rows, h * 128 : h * 128 + 128] = jnp.where(lane[:rows] < 64, left, right)

        for k in range(10):
            if k < 8 and k % 2 == 0:
                first[k // 2].wait()
            if k == 8:
                for one in first[4:]:
                    one.wait()
            ref, at = (down_s, k * B) if k < 8 else (mixed_s, (k - 8) * B)
            spread(ref, B, AT_DOWN - CUT + k * B, lambda ref, lanes: ref[at : at + B, lanes])

        def last(refs, at):
            n = jnp.broadcast_to(refs[0][0:1, at] * 0.5, (8, 128))
            b = jnp.broadcast_to(refs[1][0:1, at] * 0.5, (8, 128))
            return jnp.where(row == 0, n, jnp.where(row == 1, b, 0.0))

        spread((norm_s, bias_s), 8, AT_LAST - CUT, last)
        for one in rest:
            one.wait()

    f32 = jnp.float32
    up, query, key, value, *others = slopes
    blocks = [x.reshape(4, 4, B, -1) for x in (up, query, key)]
    return pl.pallas_call(
        kernel,
        in_specs=[SM] + [HB] * 8,
        out_specs=(VM, VM),
        out_shape=(pltpu.VMEM((n, 4, 3 * B, 256), f32), pltpu.VMEM((n, ROWS - CUT, 256), f32)),
        scratch_shapes=[
            pltpu.VMEM((512, 1024), f32),
            pltpu.VMEM((128, 1024), f32),
            pltpu.VMEM((1, 1024), f32),
            pltpu.VMEM((1, 1024), f32),
            pltpu.SemaphoreType.DMA((7 + 8 * n,)),
        ],
        compiler_params=PARAMS,
    )(place, *[hbm(x) for x in (*blocks, value[0], *others)])


def turn_kernel(at_ref, a, b, out):
    for s in range(4):
        e = pl.ds((s - at_ref[1]) & 3, 1)
        for k in range(6):
            at = s * 192 + k // 2 * B
            out[e, k * B : k * B + B, :] = a[at : at + B, k % 2 * 128 : k % 2 * 128 + 128][None]
        at = s // 2 * B
        out[e, 6 * B : 7 * B, :] = b[at : at + B, s % 2 * 128 : s % 2 * 128 + 128][None]
    at = AT_DOWN - CUT
    for h in range(2):
        lanes = slice(h * 128, h * 128 + 128)
        tiles = [b[at + k * 128 : at + k * 128 + 128, lanes].T for k in range(5)]
        last = b[AT_LAST - CUT :, lanes]
        for j in range(2):
            e = (2 * h + j - at_ref[1]) & 3
            for k, tile in enumerate(tiles):
                out[pl.ds(e, 1), (7 + k) * B : (8 + k) * B, :] = tile[None, j * B : j * B + B]
            out[pl.ds(e, 1), 12 * B :, :] = (last if j == 0 else pltpu.roll(last, 64, 1))[None]


def turn(place, a, b):
    return pl.pallas_call(
        turn_kernel,
        in_specs=[SM, VM, VM],
        out_specs=VM,
        out_shape=pltpu.VMEM((4, T, 128), jnp.float32),
        compiler_params=PARAMS,
        name="turn",
    )(place, vmem(a), vmem(b))


def norms_kernel(total, p_up, p_query, p_key, p_value, p_down, p_mixed, part):
    lane = lax.broadcasted_iota(jnp.int32, (B, 128), 1)
    params = (p_up, p_query, p_key, p_value, p_down, p_mixed)
    table = jnp.zeros((B, 128), jnp.float32)
    for m, (col, n) in enumerate(COLS):
        squares = jnp.zeros((B, 128), jnp.float32)
        own = jnp.zeros((B, 128), jnp.float32)
        for k in range(n):
            x = total[(col + k) * B : (col + k + 1) * B, :] * (1.0 / SCALE)
            squares = squares + x * x
            p = params[m][:, k * 128 : k * 128 + 128]
            own = own + p * p
        s = jnp.sum(squares, axis=1, keepdims=True)
        o = jnp.sum(own, axis=1, keepdims=True)
        table = jnp.where(lane == m, o, jnp.where(lane == 8 + m, s, table))
    table = jnp.concatenate([table, jnp.zeros((128 - B, 128), jnp.float32)], axis=0)
    table = table.T[:16, :]
    for r in range(part.shape[0]):
        part[r] = table


def norms(copies, total, *params):
    return pl.pallas_call(
        norms_kernel,
        in_specs=[VM] * 7,
        out_specs=VM,
        out_shape=pltpu.VMEM((copies, 16, 128), jnp.float32),
        compiler_params=PARAMS,
        name="norms",
    )(vmem(total), *params)


def steps(parts, total, params, states, store, store_half):
    sums = parts[0]
    for d in range(1, parts.shape[0]):
        sums = sums + parts[d]
    ratio = jnp.sqrt(sums[:8]) * lax.rsqrt(sums[8:16] + 1e-06)
    ratio = jnp.concatenate([ratio, jnp.zeros((120, 128), jnp.float32)], axis=0).T[:B, :]

    def step(m, param, state):
        new = hold_rate * state + (1.0 - hold_rate) * m * m
        return param - learn_rate * m * lax.rsqrt(new + 1e-06), new

    for i, (col, n) in enumerate(COLS):
        r = ratio[:, i : i + 1]
        for k in range(n):
            at = (col + k) * B
            lanes = slice(k * 128, k * 128 + 128)
            m = total[at : at + B, :] * (1.0 / SCALE) * r
            nxt, new = step(m, params[i][:, lanes], states[i][:, lanes])
            store(i, lanes, nxt, new)
            store_half(at, nxt)
    both = []
    for j in range(2):
        m = total[12 * B + j : 12 * B + j + 1, :B] * (1.0 / SCALE_VEC)
        nxt, new = step(m, params[6 + j][...], states[6 + j][...])
        store(6 + j, slice(None), nxt, new)
        both.append(jnp.concatenate([nxt, nxt], axis=1))
    row = lax.broadcasted_iota(jnp.int32, (8, 128), 0)
    n = jnp.broadcast_to(both[0], (8, 128))
    b = jnp.broadcast_to(both[1], (8, 128))
    store_half(12 * B, jnp.where(row == 0, n, jnp.where(row == 1, b, 0.0)))


def halves_kernel(parts, total, *refs):
    half = refs[16]

    def store_half(at, nxt):
        half[at : at + nxt.shape[0], :] = nxt.astype(jnp.bfloat16)

    steps(parts, total, refs[:8], refs[8:16], lambda *_: None, store_half)


def halves(parts, total, params, states):
    return pl.pallas_call(
        halves_kernel,
        in_specs=[VM] * 18,
        out_specs=VM,
        out_shape=pltpu.VMEM((T, 128), jnp.bfloat16),
        compiler_params=PARAMS,
        name="halves",
    )(vmem(parts), vmem(total), *params, *states)


def update_kernel(parts, total, *refs):
    nexts, news = refs[16:24], refs[24:32]

    def store(i, lanes, nxt, new):
        nexts[i][:, lanes] = nxt
        news[i][:, lanes] = new

    steps(parts, total, refs[:8], refs[8:16], store, lambda *_: None)


def update(parts, total, params, states):
    shapes = [jax.ShapeDtypeStruct(p.shape, jnp.float32) for p in params]
    out = pl.pallas_call(
        update_kernel,
        in_specs=[VM] * 18,
        out_shape=(*shapes, *shapes),
        compiler_params=PARAMS,
        name="update",
    )(vmem(parts), vmem(total), *params, *states)
    return out[:8], out[8:]


def early_kernel(at_ref, *refs):
    stacks = {0: refs[0:2], 1: refs[2:4], 3: refs[4:6]}
    up, query, key, value, down_s, mixed_s, vectors, up_s, query_s, key_s, value_s, rest_s, sems = refs[6:]
    for d in range(4):
        for k, e in enumerate(GATHER):
            r = block_of(at_ref, (at_ref[0] - d) & 3, (at_ref[1] - e) & 3)
            rows = pl.ds(pl.multiple_of(r * B, B), B)
            block = stacks[d][k // 3][k % 3] if d != 2 else jnp.zeros((T, 128), jnp.bfloat16)
            for c in range(4):
                up_s[rows, c * 128 : c * 128 + 128] = block[c * B : c * B + B, :]
            query_s[rows, :] = block[4 * B : 5 * B, :]
            key_s[rows, :] = block[5 * B : 6 * B, :]
            value_s[rows, :] = block[6 * B : 7 * B, :]
            rest_s[pl.ds(r, 1)] = block[7 * B :, :][None]
    pairs = ((up_s, up), (query_s, query), (key_s, key), (value_s, value))
    copies = [pltpu.make_async_copy(x, y, sems.at[k]) for k, (x, y) in enumerate(pairs)]
    for one in copies:
        one.start()
    lane = lax.broadcasted_iota(jnp.int32, (8, 128), 1)
    for p in range(8):
        lanes = slice(p * 128, p * 128 + 128)
        for k in range(5):
            tile = jnp.concatenate([rest_s[2 * p + j, k * B : k * B + B, :] for j in range(2)], axis=0).T
            if k < 4:
                down_s[k * 128 : k * 128 + 128, lanes] = tile
            else:
                mixed_s[:, lanes] = tile
        both = [rest_s[2 * p + j, 5 * B :, :].astype(jnp.float32) for j in range(2)]
        last = jnp.where(lane < B, both[0], both[1])
        vectors[p : p + 1, :] = last[0:1]
        vectors[8 + p : 9 + p, :] = last[1:2]
    for one in copies:
        one.wait()


def late_kernel(at_ref, a, b, *refs):
    up, query, key, value, down_s, mixed_s, vectors, down, mixed, up_s, thin_s, sems = refs[7:]
    copies = []

    def copy(source, target):
        copies.append(pltpu.make_async_copy(source, target, sems.at[len(copies)]))
        copies[-1].start()

    half = lax.broadcasted_iota(jnp.int32, (128, 128), 1) >> 6
    for i, e in enumerate(GATHER):
        block = (a, b)[i // 3].at[i % 3]
        r = block_of(at_ref, (at_ref[0] - 2) & 3, (at_ref[1] - e) & 3)
        rows = pl.ds(pl.multiple_of(r * B, B), B)
        for c in range(4):
            up_s[i, :, c * 128 : c * 128 + 128] = block[c * B : c * B + B, :]
        copy(up_s.at[i], up.at[rows])
        for c, target in enumerate((query, key, value)):
            thin_s[i, c] = block[(4 + c) * B : (5 + c) * B, :]
            copy(thin_s.at[i, c], target.at[rows])
        lanes = pl.ds(pl.multiple_of((r >> 1) * 128, 128), 128)
        mine = half == (r & 1)
        for k in range(5):
            one = block[(7 + k) * B : (8 + k) * B, :]
            tile = jnp.concatenate([one, one], axis=0).T.astype(jnp.float32)
            ref, to = (down_s, slice(k * 128, k * 128 + 128)) if k < 4 else (mixed_s, slice(None))
            ref[to, lanes] = jnp.where(mine, tile, ref[to, lanes].astype(jnp.float32)).astype(jnp.bfloat16)
        last = block[12 * B :, :].astype(jnp.float32)
        for k in range(2):
            to = pl.ds(k * 8 + (r >> 1), 1)
            vectors[to, :] = jnp.where(mine[0:1], last[k : k + 1], vectors[to, :])
    copy(down_s, down)
    copy(mixed_s, mixed)
    for one in copies:
        one.wait()


def unpack(place, early, late):
    bf16 = jnp.bfloat16
    shapes = ((1024, 512), (1024, 128), (1024, 128), (1024, 128), (512, 1024), (128, 1024))
    outs = [jax.ShapeDtypeStruct(s, bf16) for s in shapes]
    kept = [pltpu.VMEM(s, bf16) for s in shapes[4:]] + [pltpu.VMEM((16, 128), jnp.float32)]
    first = pl.pallas_call(
        early_kernel,
        in_specs=[SM] + [VM] * 6,
        out_specs=(*[HB] * 4, *[VM] * 3),
        out_shape=(*outs[:4], *kept),
        scratch_shapes=[
            *[pltpu.VMEM(s, bf16) for s in shapes[:4]],
            pltpu.VMEM((16, 5 * B + 8, 128), bf16),
            pltpu.SemaphoreType.DMA((4,)),
        ],
        compiler_params=PARAMS,
        name="unpack_early",
    )(place, *[vmem(x) for x in early])
    up, query, key, value, _, _, vectors, down, mixed = pl.pallas_call(
        late_kernel,
        in_specs=[SM, VM, VM] + [HB] * 4 + [VM] * 3,
        out_specs=(*[HB] * 4, *[VM] * 3, HB, HB),
        out_shape=(*outs[:4], *kept, *outs[4:]),
        input_output_aliases={3 + k: k for k in range(7)},
        scratch_shapes=[
            pltpu.VMEM((4, B, 512), bf16),
            pltpu.VMEM((4, 3, B, 128), bf16),
            pltpu.SemaphoreType.DMA((18,)),
        ],
        compiler_params=PARAMS,
        name="unpack_late",
    )(place, *[vmem(x) for x in late], *[hbm(x) for x in first[:4]], *[vmem(x) for x in first[4:]])
    return up, query, key, value, down, mixed, vectors


def local(*args):
    f16, f32, bf16 = jnp.float16, jnp.float32, jnp.bfloat16
    at = lax.axis_index("replica").astype(jnp.int32)
    core = lax.axis_index("model").astype(jnp.int32) & 1
    zi, yi = at >> 2, at & 3
    place = jnp.stack([jnp.where(core == 0, yi, zi), jnp.where(core == 0, zi, yi), core])

    def inner(xs):
        up, down, query, key, value, mixed, norm, bias = xs
        return up, query, key, value, down, mixed, norm, bias

    def turned(xs):
        up, query, key, value, down, mixed, norm, bias = inner(xs)
        return [vmem(x) for x in (up, query, key, value, down.T, mixed.T, norm[None], bias[None])]

    slopes, params, states = inner(args[:8]), turned(args[8:16]), turned(args[16:24])

    packed_a, packed_b = pack(place, slopes, ORDER[1:])
    two_a, one_a, three_a = [packed_a[o].reshape(CUT, 256) * SCALE for o in range(3)]
    two_b, one_b, three_b = [packed_b[o] * SCALE for o in range(3)]
    out = [x.astype(f16) for x in (two_a, two_b, one_b, three_a)]
    got = [send(x, 0, d) for x, d in zip(out, (1, 3, 1, 3))]
    mid_a = ((one_a + got[0].astype(f32)) * 0.5).astype(f16)
    mid_b = ((three_b + got[1].astype(f32)) * 0.5).astype(f16)
    through = send(mid_a, 0, 1), send(mid_b, 0, 3)
    later = lax.optimization_barrier((place, mid_a, mid_b))[0]
    own_a, own_b = pack(later, slopes, (0,))
    four_a = (own_a.reshape(CUT, 256) * SCALE + got[3].astype(f32) + 2.0 * through[0].astype(f32)) * 0.25
    four_b = (own_b[0] * SCALE + got[2].astype(f32) + 2.0 * through[1].astype(f32)) * 0.25
    four = turn(place, four_a, four_b)
    total = four[0] + sum(marked(four[e].astype(f16), e).astype(f32) for e in ORDER[1:])

    part = norms(lax.axis_size("model"), total, *params[:6])
    parts = lax.all_to_all(part, "model", 0, 0, tiled=True)
    half = halves(parts, total, params, states)

    row = [half] + [marked(half, e) for e in GATHER[1:]]
    own_a, own_b = jnp.stack(row[:3]), row[3][None]
    one_a, three_a = marked(own_a, 1, 0), marked(own_a, 3, 0)
    three_b, one_b = marked(own_b, 3, 0), marked(own_b, 1, 0)
    two_a, two_b = send(one_a, 0, 1), send(three_b, 0, 3)
    nexts, news = update(lax.optimization_barrier((parts, own_a, own_b))[0], total, params, states)
    up, query, key, value, down, mixed, vectors = unpack(place, (own_a, own_b, one_a, one_b, three_a, three_b), (two_a, two_b))
    vectors = vectors.astype(bf16)
    norm, bias = vectors[:8].reshape(1024), vectors[8:].reshape(1024)

    def outer(xs):
        up, query, key, value, down, mixed, norm, bias = xs
        return up, down.T, query, key, value, mixed.T, norm[0], bias[0]

    return (up, down, query, key, value, mixed, norm, bias, *outer(nexts), *outer(news))


def solution(mesh):
    cut = [P("replica", "model"), P("model", "replica")] + [P("replica", "model")] * 3
    cut += [P("model", "replica"), P("replica"), P("replica")]
    slope = [P("replica", None, "model"), P("replica", "model", None)] + [P("replica", None, "model")] * 3
    slope += [P("replica", "model", None), P("replica", None), P("replica", None)]
    half = [P(None, "model"), P("model", None)] + [P(None, "model")] * 3 + [P("model", None), P(), P()]
    return jax.shard_map(
        local,
        mesh=mesh,
        in_specs=(*slope, *cut, *cut),
        out_specs=(*half, *cut, *cut),
        check_vma=False,
    )
```
